32 devices in a mesh: ctx: 8 (over y, x, core), tp: 4 (over z).
Axes of the slice: x: 2, y: 2, z: 4, core: 2. Of those that a mesh axis runs over, the one named last changes fastest.
Arguments:
- resid: bfloat16 [16384, 4096], P('ctx', 'tp'), may hold values from -6 to 6
- sel_blocks: int32 [16], P('ctx'), may hold values from 0 to 127, as said below
- norm_gain: float32 [4096], replicated, may hold values from 0.5 to 1.5
- router_weight: float32 [4096], replicated, may hold values from -0.09375 to 0.09375
- w_query: bfloat16 [4096, 4096], P(None, 'tp'), may hold values from -0.25 to 0.25
- w_key: bfloat16 [4096, 512], P(None, 'tp'), may hold values from -4 to 4
- value_projection: bfloat16 [4096, 512], P(None, 'tp'), may hold values from -0.09375 to 0.09375
- w_out: bfloat16 [4096, 4096], P('tp'), may hold values from -0.09375 to 0.09375
Outputs:
- mixed: bfloat16 [2048, 4096], P(('ctx', 'tp'))
The draws below stay inside these ranges and needn't reach their ends.
Inputs may be any that keep to these rules, and one draw needn't show every extreme that they name: `sel_blocks`: entries 2 * c to 2 * c + 1 are 2 different numbers from c * 16 to c * 16 + 15, increasing.
All inputs are finite; a program needn't handle non-finite values.
Results may differ from the reference program's by a relative error of at most 0.0075.
Values may be sent and summed in bfloat16 or wider, within the bound.
No kernel may reach another device: no remote copies, remote signals or barrier semaphores. Data moves between devices by JAX's collectives and lax.ppermute only.
A program may use at most 128 MiB of HBM per device.

```python
import math
import jax
import jax.numpy as jnp
from jax import lax

MODEL_WIDTH = 4096
HEAD_WIDTH = 128
KEY_VALUE_HEADS = 4
QUERY_GROUP_SIZE = 8
BLK = 128
NBLK_DEV = 16
HQ = 32
SEL_DEV = 2
TOKENS = 16384
NBLK = 128
SELECTED_ROWS = 2048


def pick_blocks(key):
    devices = NBLK // NBLK_DEV
    scores = jax.random.randint(key, (devices, NBLK_DEV), 0, 1 << 20) * NBLK_DEV + jnp.arange(NBLK_DEV, dtype=jnp.int32)[None, :]
    unused, picked = lax.top_k(scores, SEL_DEV)
    picked = jnp.sort(picked, axis=1)
    return (picked + jnp.arange(devices, dtype=jnp.int32)[:, None] * NBLK_DEV).reshape(devices * SEL_DEV).astype(jnp.int32)


def draw_sel_blocks(key, part):
    return pick_blocks(jax.random.fold_in(key, 3))


def attention_weights(key):
    base_key = jax.random.fold_in(key, 7)
    initial_random_key, middle_random_key = jax.random.split(base_key, 2)
    query_lookup_table = jax.random.normal(initial_random_key, (MODEL_WIDTH, KEY_VALUE_HEADS, QUERY_GROUP_SIZE, HEAD_WIDTH), jnp.float32) / math.sqrt(MODEL_WIDTH)
    key_lookup_table = 3.0 * jax.random.normal(middle_random_key, (MODEL_WIDTH, KEY_VALUE_HEADS, HEAD_WIDTH), jnp.float32) / math.sqrt(MODEL_WIDTH)
    query_lookup_table = jnp.clip(query_lookup_table, -0.25, 0.25).reshape(MODEL_WIDTH, HQ * HEAD_WIDTH)
    key_lookup_table = jnp.clip(key_lookup_table, -4.0, 4.0).reshape(MODEL_WIDTH, KEY_VALUE_HEADS * HEAD_WIDTH)
    return (query_lookup_table, key_lookup_table)


def draw_w_query(key, part):
    return attention_weights(key)[0].astype(jnp.bfloat16)


def draw_w_key(key, part):
    return attention_weights(key)[1].astype(jnp.bfloat16)


def level_of(key, dims, cuts, smallest, top_value):
    def one(dim, blocks):
        draws = jax.random.uniform(jax.random.fold_in(jax.random.fold_in(key, 6), dim), (blocks,), jnp.float32, smallest / len(cuts), top_value / len(cuts))
        return jnp.repeat(jnp.exp(draws), dims[dim] // blocks).reshape((-1,) + (1,) * (len(dims) - dim - 1))

    factor_of = one(*cuts[0])
    for cut in cuts[1:]:
        factor_of = factor_of * one(*cut)
    return factor_of


def noise(stream_key, extent, width, bound, shards=(), held_as=jnp.bfloat16):
    factor_of = level_of(stream_key, extent, shards, -0.22, 0.18) if shards else 1.0
    array = jax.random.normal(stream_key, extent, jnp.float32) * width * factor_of
    return jnp.minimum(jnp.maximum(array, -bound), bound).astype(held_as)


def setup_inputs(seed: int = 0) -> dict:
    key_list = jax.random.split(jax.random.key(seed), 9)
    resid = noise(key_list[0], (TOKENS, MODEL_WIDTH), 1.0, 6.0, ((0, 8), (1, 4)))
    sel_blocks = draw_sel_blocks(jax.random.fold_in(key_list[8], 71), 0)
    norm_gain = jnp.clip(1.0 + 0.1 * jax.random.normal(key_list[2], (MODEL_WIDTH,), jnp.float32), 0.5, 1.5)
    router_weight = noise(key_list[3], (MODEL_WIDTH,), MODEL_WIDTH ** -0.5, 0.09375, (), jnp.float32)
    w_query = draw_w_query(jax.random.fold_in(key_list[8], 71), 0)
    w_key = draw_w_key(jax.random.fold_in(key_list[8], 71), 0)
    value_projection = noise(key_list[6], (MODEL_WIDTH, KEY_VALUE_HEADS * HEAD_WIDTH), MODEL_WIDTH ** -0.5, 0.09375, ((1, 4),))
    w_out = noise(key_list[7], (HQ * HEAD_WIDTH, MODEL_WIDTH), (HQ * HEAD_WIDTH) ** -0.5, 0.09375, ((0, 4),))
    return dict(resid=resid, sel_blocks=sel_blocks, norm_gain=norm_gain, router_weight=router_weight, w_query=w_query, w_key=w_key, value_projection=value_projection, w_out=w_out)


rope_base = 500000.0
norm_eps = 1e-05

def rotate_heads(values_in, positions, head_size):
    rows = values_in.shape[0]
    heads = values_in.shape[1] // head_size
    shaped = values_in.reshape(rows, heads, head_size)
    half_size = head_size // 2
    freqs = jnp.exp(jnp.arange(half_size, dtype=jnp.float32) * (-2.0 * math.log(rope_base) / head_size))
    angles = positions.astype(jnp.float32)[:, None] * freqs[None, :]
    cosine = jnp.cos(angles)[:, None, :]
    sine = jnp.sin(angles)[:, None, :]
    first = shaped[:, :, :half_size]
    second = shaped[:, :, half_size:]
    turned = jnp.concatenate([first * cosine - second * sine, second * cosine + first * sine], axis=2)
    return turned.reshape(rows, heads * head_size).astype(jnp.bfloat16)

def reference(resid, sel_blocks, norm_gain, router_weight, w_query, w_key, value_projection, w_out):
    position = (sel_blocks[:, None] * BLK + jnp.arange(BLK, dtype=jnp.int32)[None, :]).reshape(SELECTED_ROWS).astype(jnp.int32)
    chosen = resid[position]
    chosen_wide = chosen.astype(jnp.float32)
    inv_rms = lax.rsqrt(lax.optimization_barrier(jnp.mean(chosen_wide * chosen_wide, axis=1)) + norm_eps)
    normed = (chosen_wide * inv_rms[:, None] * norm_gain[None, :]).astype(jnp.bfloat16)
    gate = jax.nn.sigmoid(lax.optimization_barrier(jnp.sum(chosen_wide * router_weight[None, :], axis=1)))
    queries = rotate_heads(jnp.dot(normed, w_query, preferred_element_type=jnp.float32), position, HEAD_WIDTH)
    key_matrix = rotate_heads(jnp.dot(normed, w_key, preferred_element_type=jnp.float32), position, HEAD_WIDTH)
    value_matrix = jnp.dot(normed, value_projection, preferred_element_type=jnp.float32).astype(jnp.bfloat16)
    query_heads = queries.reshape(SELECTED_ROWS, HQ, HEAD_WIDTH).transpose(1, 0, 2)
    per_head_keys = key_matrix.reshape(SELECTED_ROWS, KEY_VALUE_HEADS, HEAD_WIDTH).transpose(1, 0, 2)
    per_head_values = value_matrix.reshape(SELECTED_ROWS, KEY_VALUE_HEADS, HEAD_WIDTH).transpose(1, 0, 2)
    allowed = position[None, :] <= position[:, None]
    score_scale = 1.0 / math.sqrt(HEAD_WIDTH)

    def one_head(head):
        query_one = query_heads[head]
        key_one = per_head_keys[head // QUERY_GROUP_SIZE]
        value_one = per_head_values[head // QUERY_GROUP_SIZE]
        scores = jnp.dot(query_one, key_one.T, preferred_element_type=jnp.float32) * score_scale
        scores = jnp.where(allowed, scores, -jnp.inf)
        highest = lax.optimization_barrier(jnp.max(scores, axis=1, keepdims=True))
        expd = jnp.exp(scores - highest)
        weights = expd.astype(jnp.bfloat16)
        mixed_values = jnp.dot(weights, value_one, preferred_element_type=jnp.float32)
        return (mixed_values / lax.optimization_barrier(jnp.sum(expd, axis=1, keepdims=True))).astype(jnp.bfloat16)
    per_head = lax.map(one_head, jnp.arange(HQ, dtype=jnp.int32))
    attended = per_head.transpose(1, 0, 2).reshape(SELECTED_ROWS, HQ * HEAD_WIDTH)
    projected = jnp.dot(attended, w_out, preferred_element_type=jnp.float32)
    return (chosen_wide + gate[:, None] * projected).astype(jnp.bfloat16)
```

```python
import functools
import math

import jax
import jax.numpy as jnp
from jax import lax
from jax.experimental import pallas as pl
from jax.experimental.pallas import tpu as pltpu
from jax.sharding import PartitionSpec as P

HEAD_WIDTH = 128
BLK = 128

rope_base = 500000.0
norm_eps = 1e-05
score_scale = math.log2(math.e) / math.sqrt(HEAD_WIDTH)


VMEM = pl.BlockSpec(memory_space=pltpu.VMEM)
SMEM = pl.BlockSpec(memory_space=pltpu.SMEM)
ANY = pl.BlockSpec(memory_space=pl.ANY)
BF = jnp.bfloat16
F32 = jnp.float32


def sds(shape, dtype):
    return jax.ShapeDtypeStruct(shape, dtype)


def cost(flops, nbytes):
    return pl.CostEstimate(flops=int(flops), bytes_accessed=int(nbytes), transcendentals=0)


def pick_rows(resid, local_ids, pieces):
    width = resid.shape[1]
    w = width // pieces
    picked = local_ids.shape[0]

    def kernel(ids, x_ref, *outs):
        for p, out in enumerate(outs):
            out[...] = x_ref[:, p * w : (p + 1) * w]

    return pl.pallas_call(
        kernel,
        out_shape=[sds((picked * BLK, w), BF)] * pieces,
        grid_spec=pltpu.PrefetchScalarGridSpec(
            num_scalar_prefetch=1,
            grid=(picked,),
            in_specs=[pl.BlockSpec((BLK, width), lambda i, ids: (ids[i], 0))],
            out_specs=[pl.BlockSpec((BLK, w), lambda i, ids: (i, 0))] * pieces,
        ),
        cost_estimate=cost(1 << 20, 4 * picked * BLK * width),
        name="pick",
    )(local_ids, resid)


def rotate_half(x, cos2, sin2):
    return x * cos2 + pltpu.roll(x, HEAD_WIDTH // 2, 1) * sin2


def accumulate(piece_ids, pieces, gain_rw, w_query, w_key, w_value):
    count = len(pieces)
    rows, w = pieces[0].shape
    nq, nk = w_query.shape[1], w_key.shape[1]

    def kernel(ids, gain_ref, *refs):
        xs = refs[:count]
        wq, wk, wv = refs[count : count + 3]
        q_out, kv_out, ss_out, gd_out = refs[count + 3 : count + 7]
        bq, bk, bv, sems = refs[count + 7 :]
        copies = []
        for p in range(count):
            at = pl.ds(pl.multiple_of(ids[p] * w, w), w)
            trio = [
                pltpu.make_async_copy(src.at[at, :], dst.at[p], sems.at[p, k])
                for k, (src, dst) in enumerate(((wk, bk), (wv, bv), (wq, bq)))
            ]
            for c in trio:
                c.start()
            copies.append(trio)
        ss = jnp.zeros((rows, 1), F32)
        gd = jnp.zeros((rows, 1), F32)
        for p in range(count):
            x = xs[p][...].astype(F32)
            ss += jnp.sum(x * x, axis=1, keepdims=True)
            gd += jnp.sum(x * gain_ref[ids[p], 1:2, :], axis=1, keepdims=True)
            xg = (x * gain_ref[ids[p], 0:1, :]).astype(BF)
            for c in copies[p]:
                c.wait()
            k = jnp.dot(xg, bk[p], preferred_element_type=F32)
            v = jnp.dot(xg, bv[p], preferred_element_type=F32)
            q = jnp.dot(xg, bq[p], preferred_element_type=F32)
            if p == 0:
                kv_out[:, :nk] = k
                kv_out[:, nk:] = v
                q_out[...] = q
            else:
                kv_out[:, :nk] += k
                kv_out[:, nk:] += v
                q_out[...] += q
        ss_out[...] = ss
        gd_out[...] = gd

    return pl.pallas_call(
        kernel,
        out_shape=[
            sds((rows, nq), F32),
            sds((rows, 2 * nk), F32),
            sds((rows, 1), F32),
            sds((rows, 1), F32),
        ],
        in_specs=[SMEM, VMEM] + [VMEM] * count + [ANY] * 3,
        out_specs=[VMEM] * 4,
        scratch_shapes=[
            pltpu.VMEM((count, w, nq), BF),
            pltpu.VMEM((count, w, nk), BF),
            pltpu.VMEM((count, w, nk), BF),
            pltpu.SemaphoreType.DMA((count, 3)),
        ],
        cost_estimate=cost(2 * rows * w * count * (nq + 2 * nk), 2 * count * w * (nq + 2 * nk)),
        compiler_params=pltpu.CompilerParams(vmem_limit_bytes=48 << 20),
        name="accumulate",
    )(piece_ids, gain_rw, *pieces, w_query, w_key, w_value)


def finish(piece_ids, pieces, gain_rw, w_query, w_key, w_value, partial, cos2, sin2, features):
    count = len(pieces)
    rows, w = pieces[0].shape
    nq, nk = w_query.shape[1], w_key.shape[1]

    def kernel(ids, gain_ref, *refs):
        xs = refs[:count]
        wq, wk, wv, qa, kva, ssa, gda, cos_ref, sin_ref = refs[count : count + 9]
        q_out, kv_out, gate_out = refs[count + 9 : count + 12]
        bq, bk, bv, sems = refs[count + 12 :]
        copies = []
        for p in range(count):
            at = pl.ds(pl.multiple_of(ids[p] * w, w), w)
            trio = [
                pltpu.make_async_copy(src.at[at, :], dst.at[p], sems.at[p, k])
                for k, (src, dst) in enumerate(((wk, bk), (wv, bv), (wq, bq)))
            ]
            for c in trio:
                c.start()
            copies.append(trio)
        ss = ssa[...]
        gd = gda[...]
        gained = []
        for p in range(count):
            x = xs[p][...].astype(F32)
            ss += jnp.sum(x * x, axis=1, keepdims=True)
            gd += jnp.sum(x * gain_ref[ids[p], 1:2, :], axis=1, keepdims=True)
            gained.append((x * gain_ref[ids[p], 0:1, :]).astype(BF))
        inv = lax.rsqrt(ss * (1.0 / features) + norm_eps)
        gate_out[...] = jnp.broadcast_to(1.0 / (1.0 + jnp.exp(-gd)), gate_out.shape)
        cos2 = cos_ref[...] * inv
        sin2 = sin_ref[...] * inv
        for p in range(count):
            copies[p][0].wait()
            copies[p][1].wait()
        k, v = kva[:, :nk], kva[:, nk:]
        for p in range(count):
            k += jnp.dot(gained[p], bk[p], preferred_element_type=F32)
            v += jnp.dot(gained[p], bv[p], preferred_element_type=F32)
        for h in range(nk // HEAD_WIDTH):
            at = slice(h * HEAD_WIDTH, (h + 1) * HEAD_WIDTH)
            kv_out[:, at] = rotate_half(k[:, at], cos2, sin2).astype(BF)
        kv_out[:, nk:] = (v * inv).astype(BF)
        cosq = cos2 * score_scale
        sinq = sin2 * score_scale
        for p in range(count):
            copies[p][2].wait()
        for h in range(0, nq // HEAD_WIDTH, 2):
            both = slice(h * HEAD_WIDTH, (h + 2) * HEAD_WIDTH)
            q = qa[:, both]
            for p in range(count):
                q += jnp.dot(gained[p], bq[p, :, both], preferred_element_type=F32)
            for i in range(2):
                at = slice(i * HEAD_WIDTH, (i + 1) * HEAD_WIDTH)
                to = slice((h + i) * HEAD_WIDTH, (h + i + 1) * HEAD_WIDTH)
                q_out[:, to] = rotate_half(q[:, at], cosq, sinq).astype(BF)

    return pl.pallas_call(
        kernel,
        out_shape=[
            sds((rows, nq), BF),
            sds((rows, 2 * nk), BF),
            sds((rows, HEAD_WIDTH), F32),
        ],
        in_specs=[SMEM, VMEM] + [VMEM] * count + [ANY] * 3 + [VMEM] * 6,
        out_specs=[VMEM] * 3,
        scratch_shapes=[
            pltpu.VMEM((count, w, nq), BF),
            pltpu.VMEM((count, w, nk), BF),
            pltpu.VMEM((count, w, nk), BF),
            pltpu.SemaphoreType.DMA((count, 3)),
        ],
        cost_estimate=cost(2 * rows * w * count * (nq + 2 * nk), 2 * count * w * (nq + 2 * nk)),
        compiler_params=pltpu.CompilerParams(vmem_limit_bytes=40 << 20),
        name="finish",
    )(piece_ids, gain_rw, *pieces, w_query, w_key, w_value, *partial, cos2, sin2)


def attend(meta, q, kv, w_out, share, chunks, dtypes):
    dests = len(dtypes)
    rows, nq = q.shape
    heads = nq // HEAD_WIDTH
    nk = kv.shape[1] // 2
    kv_heads = nk // HEAD_WIDTH
    group = heads // kv_heads
    part = dests * share
    tall = group * part
    model = w_out.shape[1]
    cw = model // chunks

    def kernel(meta_ref, q_ref, kv_ref, w_hbm, *refs):
        outs = refs[: dests * chunks]
        qs, vs, m_ref, acc, att, wv, sems = refs[dests * chunks :]
        copies = [
            pltpu.make_async_copy(
                w_hbm.at[:, i * cw : (i + 1) * cw], wv.at[i], sems.at[i]
            )
            for i in range(chunks)
        ]
        for c in copies:
            c.start()
        me = meta_ref[0]
        vs[:, HEAD_WIDTH:] = jnp.ones((rows, HEAD_WIDTH), BF)
        for kh in range(kv_heads):
            for h in range(group):
                col = (kh * group + h) * HEAD_WIDTH
                for d in range(dests):
                    src = pl.ds(pl.multiple_of(meta_ref[1 + d] * share, share), share)
                    to = h * part + d * share
                    qs[to : to + share, :] = q_ref[src, col : col + HEAD_WIDTH]
            k_at = slice(kh * HEAD_WIDTH, (kh + 1) * HEAD_WIDTH)
            v_at = slice(nk + kh * HEAD_WIDTH, nk + (kh + 1) * HEAD_WIDTH)

            def scores_of(block):
                at = pl.ds(pl.multiple_of(block * rows, rows), rows)
                vs[:, :HEAD_WIDTH] = kv_ref[at, v_at]
                return lax.dot_general(
                    qs[...],
                    kv_ref[at, k_at],
                    (((1,), (1,)), ((), ())),
                    preferred_element_type=F32,
                )

            s = scores_of(me)
            row = lax.broadcasted_iota(jnp.int32, (share, 1), 0)
            own_rows = jnp.concatenate(
                [row + meta_ref[1 + d] * share for d in range(dests)] * group, axis=0
            )
            key = lax.broadcasted_iota(jnp.int32, (tall, rows), 1)
            s = jnp.where(key <= own_rows, s, -1e30)
            m = jnp.max(s, axis=1, keepdims=True)
            m_ref[...] = jnp.broadcast_to(m, m_ref.shape)
            acc[...] = jnp.dot(
                jnp.exp2(s - m).astype(BF), vs[...], preferred_element_type=F32
            )

            def fold(block, unused):
                s = scores_of(block)
                old = m_ref[:, 0:1]
                m = jnp.maximum(old, jnp.max(s, axis=1, keepdims=True))
                m_ref[...] = jnp.broadcast_to(m, m_ref.shape)
                acc[...] = acc[...] * jnp.exp2(old - m) + jnp.dot(
                    jnp.exp2(s - m).astype(BF), vs[...], preferred_element_type=F32
                )
                return unused

            lax.fori_loop(0, me, fold, 0)
            done = (acc[:, :HEAD_WIDTH] / acc[:, HEAD_WIDTH:]).astype(BF)
            for h in range(group):
                col = (kh * group + h) * HEAD_WIDTH
                att[:, col : col + HEAD_WIDTH] = done[h * part : (h + 1) * part, :]
        for i in range(chunks):
            copies[i].wait()
            proj = jnp.dot(att[...], wv[i], preferred_element_type=F32)
            for d in range(dests):
                out = outs[d * chunks + i]
                out[...] = proj[d * share : (d + 1) * share, :].astype(out.dtype)

    return pl.pallas_call(
        kernel,
        out_shape=[sds((share, cw), dtypes[d][i]) for d in range(dests) for i in range(chunks)],
        in_specs=[SMEM, VMEM, VMEM, ANY],
        out_specs=[VMEM] * (dests * chunks),
        scratch_shapes=[
            pltpu.VMEM((tall, HEAD_WIDTH), BF),
            pltpu.VMEM((rows, 2 * HEAD_WIDTH), BF),
            pltpu.VMEM((tall, HEAD_WIDTH), F32),
            pltpu.VMEM((tall, 2 * HEAD_WIDTH), F32),
            pltpu.VMEM((part, nq), BF),
            pltpu.VMEM((chunks, nq, cw), BF),
            pltpu.SemaphoreType.DMA((chunks,)),
        ],
        cost_estimate=cost(
            4 * part * nq * kv.shape[0] + 2 * part * nq * model, 2 * nq * model + 2 * kv.size
        ),
        compiler_params=pltpu.CompilerParams(vmem_limit_bytes=48 << 20),
        name="attend",
    )(meta, q, kv, w_out)


def combine(meta, pieces, gate, got, own, share):
    count = len(pieces)
    w = pieces[0].shape[1]
    chunks = len(got)
    cw = got[0].shape[1]
    model = chunks * cw

    def kernel(meta_ref, *refs):
        xs = refs[:count]
        gate_ref = refs[count]
        gs = refs[count + 1 : count + 1 + chunks]
        os = refs[count + 1 + chunks : count + 1 + 2 * chunks]
        out, tmp = refs[count + 1 + 2 * chunks :]
        for i in range(chunks):
            tmp[:, i * cw : (i + 1) * cw] = gs[i][...].astype(F32) + os[i][...]
        g = gate_ref[:, 0:1]
        for p in range(count):
            at = pl.ds(pl.multiple_of(meta_ref[1 + p] * w, w), w)
            out[:, at] = (xs[p][...].astype(F32) + g * tmp[:, at]).astype(BF)

    row = lambda i, m: (m[0], 0)
    whole = lambda i, m: (0, 0)
    return pl.pallas_call(
        kernel,
        out_shape=sds((share, model), BF),
        grid_spec=pltpu.PrefetchScalarGridSpec(
            num_scalar_prefetch=1,
            grid=(1,),
            in_specs=[pl.BlockSpec((share, w), row)] * count
            + [pl.BlockSpec((share, HEAD_WIDTH), row)]
            + [pl.BlockSpec((share, cw), whole)] * (2 * chunks),
            out_specs=pl.BlockSpec((share, model), whole),
            scratch_shapes=[pltpu.VMEM((share, model), F32)],
        ),
        cost_estimate=cost(1 << 20, 8 * share * model),
        name="combine",
    )(meta, *pieces, gate, *got, *own)


def on_device(resid, sel_blocks, norm_gain, router_weight, w_query, w_key, value_projection, w_out):
    picked = sel_blocks.shape[0]
    local_rows, local_width = resid.shape
    block_count = local_rows // BLK
    n = lax.axis_size("tp")
    t = lax.axis_index("tp")
    c = lax.axis_index("ctx")
    rows = picked * BLK
    share = rows // n
    features = local_width * n
    per_way = 2
    chains = 2 * per_way
    w = local_width // chains
    up = [(i, (i + 1) % n) for i in range(n)]
    down = [(i, (i - 1) % n) for i in range(n)]
    ways = [up if k % 2 == 0 else down for k in range(chains)]

    local_ids = sel_blocks - c * block_count
    held = pick_rows(resid, local_ids, chains)

    positions = (sel_blocks[:, None] * BLK + jnp.arange(BLK, dtype=jnp.int32)[None, :]).reshape(rows)
    half = HEAD_WIDTH // 2
    freqs = jnp.exp(jnp.arange(half, dtype=F32) * (-2.0 * math.log(rope_base) / HEAD_WIDTH))
    angles = positions.astype(F32)[:, None] * freqs[None, :]
    cos, sin = jnp.cos(angles), jnp.sin(angles)
    cos2 = jnp.concatenate([cos, cos], axis=1)
    sin2 = jnp.concatenate([-sin, sin], axis=1)
    gain_rw = jnp.stack(
        [norm_gain.reshape(-1, w), router_weight.reshape(-1, w)], axis=1
    )

    stages = [held]
    for s in range(n - 1):
        held = [lax.ppermute(b, "tp", ways[k]) for k, b in enumerate(held)]
        stages.append(held)
    ids = []
    for s in range(n):
        for k in range(chains):
            level = lax.rem(t - s + n, n) if k % 2 == 0 else lax.rem(t + s, n)
            ids.append(level * chains + k)
    pieces = [b for stage in stages for b in stage]
    first = chains * (n - 1)
    partial = accumulate(
        jnp.stack(ids[:first]), pieces[:first], gain_rw, w_query, w_key, value_projection
    )
    q, kv, gate = finish(
        jnp.stack(ids[first:]), pieces[first:], gain_rw, w_query, w_key, value_projection,
        partial, cos2, sin2, features,
    )
    kv_all = lax.all_gather(kv, "ctx", axis=0, tiled=True)

    order = [lax.rem(t + n - 1, n), lax.rem(t + 1, n)]
    rest = [lax.rem(t + d, n) for d in range(2, n - 1)] + [t]
    out_ways = [up, down] * per_way
    chunks = len(out_ways)
    near = attend(
        jnp.stack([c] + order), q, kv_all, w_out, share, chunks,
        [[BF if k % 2 == d else F32 for k in range(chunks)] for d in range(2)],
    )
    far = attend(
        jnp.stack([c] + rest), q, kv_all, w_out, share, chunks, [[F32] * chunks] * len(rest)
    )

    def part_of(offset, k):
        offset = offset % n
        if offset == n - 1:
            return near[k]
        if offset == 1:
            return near[chunks + k]
        return far[((offset - 2) if offset else len(rest) - 1) * chunks + k]

    moving = [part_of(-1 if k % 2 == 0 else 1, k) for k in range(chunks)]
    for s in range(1, n):
        moving = [lax.ppermute(b, "tp", out_ways[k]) for k, b in enumerate(moving)]
        if s < n - 1:
            moving = [
                (b.astype(F32) + part_of(-1 - s if k % 2 == 0 else 1 + s, k)).astype(BF)
                for k, b in enumerate(moving)
            ]
    own = [part_of(0, k) for k in range(chunks)]
    return combine(jnp.stack([t] + ids), pieces, gate, moving, own, share)


def solution(mesh):
    return jax.shard_map(
        on_device,
        mesh=mesh,
        in_specs=(
            P("ctx", "tp"),
            P("ctx"),
            P(),
            P(),
            P(None, "tp"),
            P(None, "tp"),
            P(None, "tp"),
            P("tp", None),
        ),
        out_specs=P(("ctx", "tp"), None),
        check_vma=False,
    )
```

```python
import math

import jax
import jax.numpy as jnp
from jax import lax
from jax.experimental import pallas as pl
from jax.experimental.pallas import tpu as pltpu
from jax.sharding import PartitionSpec as P

HEAD_WIDTH = 128
BLK = 128

rope_base = 500000.0
norm_eps = 1e-05
score_scale = math.log2(math.e) / math.sqrt(HEAD_WIDTH)

GATHER_WAYS = 2
SCATTER_WAYS = 2


VMEM = pl.BlockSpec(memory_space=pltpu.VMEM)
SMEM = pl.BlockSpec(memory_space=pltpu.SMEM)
HBM = pl.BlockSpec(memory_space=pltpu.HBM)
BF = jnp.bfloat16
F32 = jnp.float32


def sds(shape, dtype):
    return jax.ShapeDtypeStruct(shape, dtype)


def cost(flops, nbytes):
    return pl.CostEstimate(flops=int(flops), bytes_accessed=int(nbytes), transcendentals=0)


def in_hbm(x):
    return pltpu.with_memory_space_constraint(x, pltpu.HBM)


def params(mib):
    return pltpu.CompilerParams(vmem_limit_bytes=mib << 20)


def pick_rows(resid, sel_blocks, pieces):
    local_rows, width = resid.shape
    w = width // pieces
    picked = sel_blocks.shape[0]
    block_count = local_rows // BLK

    def kernel(sel, x_hbm, *refs):
        outs, sems = refs[:pieces], refs[pieces]
        copies = []
        for i in range(picked):
            at = pl.ds(pl.multiple_of(lax.rem(sel[i], block_count) * BLK, BLK), BLK)
            for p in range(pieces):
                copies.append(
                    pltpu.make_async_copy(
                        x_hbm.at[at, p * w : (p + 1) * w],
                        outs[p].at[i * BLK : (i + 1) * BLK, :],
                        sems.at[i, p],
                    )
                )
        for c in copies:
            c.start()
        for c in copies:
            c.wait()

    return pl.pallas_call(
        kernel,
        out_shape=[sds((picked * BLK, w), BF)] * pieces,
        in_specs=[SMEM, HBM],
        out_specs=[VMEM] * pieces,
        scratch_shapes=[pltpu.SemaphoreType.DMA((picked, pieces))],
        cost_estimate=cost(1 << 20, 4 * picked * BLK * width),
        compiler_params=params(8),
        name="pick",
    )(sel_blocks, in_hbm(resid))


def rotate_half(x, cos2, sin2):
    return x * cos2 + pltpu.roll(x, HEAD_WIDTH // 2, 1) * sin2


def piece_index(stage, k, n, chains):
    t = lax.axis_index("tp")
    level = lax.rem(t - stage + n, n) if k % 2 == 0 else lax.rem(t + stage, n)
    return level * chains + k


def gained(x, at, gain_ref):
    return (x.astype(F32) * gain_ref[:, at]).astype(BF)


def fetch(sources, buffers, sems, offsets, w):
    out = []
    for p, off in enumerate(offsets):
        row = [
            pltpu.make_async_copy(src.at[pl.ds(off, w), :], dst.at[p], sems.at[p, i])
            for i, (src, dst) in enumerate(zip(sources, buffers))
        ]
        for c in row:
            c.start()
        out.append(row)
    return out


def accumulate(stage, n, pieces, gain, router, weights, state, share):
    count = len(pieces)
    rows, w = pieces[0].shape
    wq, wk, wv = weights
    nq, nk = wq.shape[1], wk.shape[1]
    features = gain.shape[1]
    held = 0 if state is None else len(state)

    def kernel(*refs):
        xs = refs[:count]
        gain_ref, router_ref, wqr, wkr, wvr = refs[count : count + 5]
        before = refs[count + 5 : count + 5 + held]
        q_out, k_out, v_out, ss_out, gd_out, own_out = refs[count + 5 + held : count + 11 + held]
        bk, bv, bq, sems = refs[count + 11 + held :]
        offsets = [
            pl.multiple_of(piece_index(stage, p, n, count) * w, w) for p in range(count)
        ]
        copies = fetch((wkr, wvr, wqr), (bk, bv, bq), sems, offsets, w)
        first = pl.multiple_of(lax.axis_index("tp") * share, share)
        k = v = None
        xg = []
        ss = gd = None
        for p in range(count):
            at = pl.ds(offsets[p], w)
            x = xs[p][...].astype(F32)
            a = jnp.sum(x * x, axis=1, keepdims=True)
            b = jnp.sum(x * router_ref[:, at], axis=1, keepdims=True)
            ss = a if ss is None else ss + a
            gd = b if gd is None else gd + b
            xg.append((x * gain_ref[:, at]).astype(BF))
            own_out[:, at] = xs[p][pl.ds(first, share), :]
        for p in range(count):
            for c in copies[p]:
                c.wait()
        for ref, out, buf in ((0, q_out, bq), (1, k_out, bk), (2, v_out, bv)):
            total = before[ref][...] if held else None
            for p in range(count):
                d = jnp.dot(xg[p], buf[p], preferred_element_type=F32)
                total = d if total is None else total + d
            out[...] = total
        ss_out[...] = ss + before[3][...] if held else ss
        gd_out[...] = gd + before[4][...] if held else gd

    shapes = [
        sds((rows, nq), F32),
        sds((rows, nk), F32),
        sds((rows, nk), F32),
        sds((rows, 1), F32),
        sds((rows, 1), F32),
        sds((share, features), BF),
    ]
    return pl.pallas_call(
        kernel,
        out_shape=shapes,
        in_specs=[VMEM] * (count + 2) + [HBM] * 3 + [VMEM] * held,
        out_specs=[VMEM] * 6,
        scratch_shapes=[
            pltpu.VMEM((count, w, nk), BF),
            pltpu.VMEM((count, w, nk), BF),
            pltpu.VMEM((count, w, nq), BF),
            pltpu.SemaphoreType.DMA((count, 3)),
        ],
        input_output_aliases={count + 5 + i: i for i in range(held)},
        cost_estimate=cost(2 * rows * w * count * (nq + 2 * nk), 2 * count * w * (nq + 2 * nk)),
        compiler_params=params(16),
        name="accumulate",
    )(*pieces, gain, router, *map(in_hbm, weights), *(state or ()))


def finish_kv(stage, n, pieces, gain, router, weights, state, cos2, sin2):
    count = len(pieces)
    rows, w = pieces[0].shape
    wq, wk, wv = weights
    nk = wk.shape[1]
    features = gain.shape[1]

    def kernel(*refs):
        xs = refs[:count]
        gain_ref, router_ref, wkr, wvr, ka, va, ssa, gda, cos_ref, sin_ref = refs[
            count : count + 10
        ]
        kv_out, inv_out, gate_out, bk, bv, sems = refs[count + 10 :]
        offsets = [
            pl.multiple_of(piece_index(stage, p, n, count) * w, w) for p in range(count)
        ]
        copies = fetch((wkr, wvr), (bk, bv), sems, offsets, w)
        ss, gd = ssa[...], gda[...]
        xg = []
        for p in range(count):
            at = pl.ds(offsets[p], w)
            x = xs[p][...].astype(F32)
            ss += jnp.sum(x * x, axis=1, keepdims=True)
            gd += jnp.sum(x * router_ref[:, at], axis=1, keepdims=True)
            xg.append((x * gain_ref[:, at]).astype(BF))
        inv = jnp.broadcast_to(lax.rsqrt(ss * (1.0 / features) + norm_eps), (rows, HEAD_WIDTH))
        inv_out[...] = inv
        gate_out[...] = jnp.broadcast_to(1.0 / (1.0 + jnp.exp(-gd)), gate_out.shape)
        k, v = ka[...], va[...]
        for p in range(count):
            for c in copies[p]:
                c.wait()
            k += jnp.dot(xg[p], bk[p], preferred_element_type=F32)
            v += jnp.dot(xg[p], bv[p], preferred_element_type=F32)
        cos, sin = cos_ref[...] * inv, sin_ref[...] * inv
        for h in range(nk // HEAD_WIDTH):
            at = slice(h * HEAD_WIDTH, (h + 1) * HEAD_WIDTH)
            to = slice(nk + h * HEAD_WIDTH, nk + (h + 1) * HEAD_WIDTH)
            kv_out[:, at] = rotate_half(k[:, at], cos, sin).astype(BF)
            kv_out[:, to] = (v[:, at] * inv).astype(BF)

    return pl.pallas_call(
        kernel,
        out_shape=[
            sds((rows, 2 * nk), BF),
            sds((rows, HEAD_WIDTH), F32),
            sds((rows, HEAD_WIDTH), F32),
        ],
        in_specs=[VMEM] * (count + 2) + [HBM] * 2 + [VMEM] * 6,
        out_specs=[VMEM] * 3,
        scratch_shapes=[
            pltpu.VMEM((count, w, nk), BF),
            pltpu.VMEM((count, w, nk), BF),
            pltpu.SemaphoreType.DMA((count, 2)),
        ],
        cost_estimate=cost(4 * rows * w * count * nk, 4 * count * w * nk),
        compiler_params=params(8),
        name="finish_kv",
    )(*pieces, gain, router, in_hbm(wk), in_hbm(wv), state[1], state[2], state[3], state[4], cos2, sin2)


def finish_q(stage, n, pieces, gain, weights, state, inv, cos2, sin2, share):
    count = len(pieces)
    rows, w = pieces[0].shape
    wq = weights[0]
    nq = wq.shape[1]
    features = gain.shape[1]

    def kernel(*refs):
        xs = refs[:count]
        gain_ref, wqr, qa, own_in, inv_ref, cos_ref, sin_ref = refs[count : count + 7]
        q_out, own_out, bq, sems = refs[count + 7 :]
        offsets = [
            pl.multiple_of(piece_index(stage, p, n, count) * w, w) for p in range(count)
        ]
        copies = fetch((wqr,), (bq,), sems, offsets, w)
        first = pl.multiple_of(lax.axis_index("tp") * share, share)
        xg = []
        for p in range(count):
            at = pl.ds(offsets[p], w)
            xg.append((xs[p][...].astype(F32) * gain_ref[:, at]).astype(BF))
            own_out[:, at] = xs[p][pl.ds(first, share), :]
        factor = inv_ref[...] * score_scale
        cos, sin = cos_ref[...] * factor, sin_ref[...] * factor
        for p in range(count):
            copies[p][0].wait()
        for h in range(0, nq, 2 * HEAD_WIDTH):
            both = slice(h, h + 2 * HEAD_WIDTH)
            q = qa[:, both]
            for p in range(count):
                q += jnp.dot(xg[p], bq[p, :, both], preferred_element_type=F32)
            for i in range(2):
                at = slice(i * HEAD_WIDTH, (i + 1) * HEAD_WIDTH)
                to = slice(h + i * HEAD_WIDTH, h + (i + 1) * HEAD_WIDTH)
                q_out[:, to] = rotate_half(q[:, at], cos, sin).astype(BF)

    return pl.pallas_call(
        kernel,
        out_shape=[sds((rows, nq), BF), sds((share, features), BF)],
        in_specs=[VMEM] * (count + 1) + [HBM] + [VMEM] * 5,
        out_specs=[VMEM] * 2,
        scratch_shapes=[
            pltpu.VMEM((count, w, nq), BF),
            pltpu.SemaphoreType.DMA((count, 1)),
        ],
        input_output_aliases={count + 3: 1},
        cost_estimate=cost(2 * rows * w * count * nq, 2 * count * w * nq),
        compiler_params=params(12),
        name="finish_q",
    )(*pieces, gain, in_hbm(wq), state[0], state[5], inv, cos2, sin2)


def attend(q, blocks, w_out, share, offsets, chunks, dtypes):
    n = lax.axis_size("tp")
    dests = len(offsets)
    rows, nq = q.shape
    heads = nq // HEAD_WIDTH
    nk = blocks[0].shape[1] // 2
    kv_heads = nk // HEAD_WIDTH
    group = heads // kv_heads
    part = dests * share
    tall = group * part
    model = w_out.shape[1]
    cw = model // chunks
    spans = len(blocks)

    def kernel(*refs):
        q_ref = refs[0]
        kvs = refs[1 : 1 + spans]
        w_hbm = refs[1 + spans]
        outs = refs[2 + spans : 2 + spans + dests * chunks]
        qs, vs, sc, m_ref, acc, att, wv, sems = refs[2 + spans + dests * chunks :]
        copies = [
            pltpu.make_async_copy(w_hbm.at[:, i * cw : (i + 1) * cw], wv.at[i], sems.at[i])
            for i in range(chunks)
        ]
        for c in copies:
            c.start()
        me = lax.axis_index("ctx")
        t = lax.axis_index("tp")
        starts = [
            pl.multiple_of(lax.rem(t + off, n) * share, share) for off in offsets
        ]
        vs[:, HEAD_WIDTH:] = jnp.ones((rows, HEAD_WIDTH), BF)
        for kh in range(kv_heads):
            for h in range(group):
                col = (kh * group + h) * HEAD_WIDTH
                for d in range(dests):
                    to = h * part + d * share
                    qs[to : to + share, :] = q_ref[pl.ds(starts[d], share), col : col + HEAD_WIDTH]
            k_at = slice(kh * HEAD_WIDTH, (kh + 1) * HEAD_WIDTH)
            v_at = slice(nk + kh * HEAD_WIDTH, nk + (kh + 1) * HEAD_WIDTH)

            def score(k):
                return lax.dot_general(
                    qs[...],
                    kvs[k][:, k_at],
                    (((1,), (1,)), ((), ())),
                    preferred_element_type=F32,
                )

            row = lax.broadcasted_iota(jnp.int32, (share, 1), 0)
            own_rows = jnp.concatenate([row + s for s in starts] * group, axis=0)
            key = lax.broadcasted_iota(jnp.int32, (tall, rows), 1)
            s = jnp.where(key <= own_rows, score(0), -1e30)
            sc[0] = s
            m_ref[...] = jnp.maximum(s[:, :HEAD_WIDTH], s[:, HEAD_WIDTH : 2 * HEAD_WIDTH])
            for i in range(2, rows // HEAD_WIDTH):
                m_ref[...] = jnp.maximum(m_ref[...], s[:, i * HEAD_WIDTH : (i + 1) * HEAD_WIDTH])
            for k in range(1, spans):

                @pl.when((me ^ k) < me)
                def _():
                    s = score(k)
                    sc[k] = s
                    m = m_ref[...]
                    for i in range(rows // HEAD_WIDTH):
                        m = jnp.maximum(m, s[:, i * HEAD_WIDTH : (i + 1) * HEAD_WIDTH])
                    m_ref[...] = m

            m_ref[...] = jnp.broadcast_to(
                jnp.max(m_ref[...], axis=1, keepdims=True), m_ref.shape
            )

            def weigh(k):
                vs[:, :HEAD_WIDTH] = kvs[k][:, v_at]
                m = m_ref[...]
                p = jnp.concatenate(
                    [
                        jnp.exp2(sc[k, :, i * HEAD_WIDTH : (i + 1) * HEAD_WIDTH] - m).astype(BF)
                        for i in range(rows // HEAD_WIDTH)
                    ],
                    axis=1,
                )
                return jnp.dot(p, vs[...], preferred_element_type=F32)

            acc[...] = weigh(0)
            for k in range(1, spans):

                @pl.when((me ^ k) < me)
                def _():
                    acc[...] += weigh(k)

            done = (acc[:, :HEAD_WIDTH] / acc[:, HEAD_WIDTH:]).astype(BF)
            for h in range(group):
                col = (kh * group + h) * HEAD_WIDTH
                att[:, col : col + HEAD_WIDTH] = done[h * part : (h + 1) * part, :]
        for i in range(chunks):
            copies[i].wait()
            proj = jnp.dot(att[...], wv[i], preferred_element_type=F32)
            for d in range(dests):
                out = outs[d * chunks + i]
                out[...] = proj[d * share : (d + 1) * share, :].astype(out.dtype)

    return pl.pallas_call(
        kernel,
        out_shape=[sds((share, cw), dtypes[d][i]) for d in range(dests) for i in range(chunks)],
        in_specs=[VMEM] * (1 + spans) + [HBM],
        out_specs=[VMEM] * (dests * chunks),
        scratch_shapes=[
            pltpu.VMEM((tall, HEAD_WIDTH), BF),
            pltpu.VMEM((rows, 2 * HEAD_WIDTH), BF),
            pltpu.VMEM((spans, tall, rows), F32),
            pltpu.VMEM((tall, HEAD_WIDTH), F32),
            pltpu.VMEM((tall, 2 * HEAD_WIDTH), F32),
            pltpu.VMEM((part, nq), BF),
            pltpu.VMEM((chunks, nq, cw), BF),
            pltpu.SemaphoreType.DMA((chunks,)),
        ],
        cost_estimate=cost(
            4 * part * nq * rows * spans + 2 * part * nq * model,
            2 * nq * model + 2 * spans * rows * nk,
        ),
        compiler_params=params(24 + spans * tall * rows * 4 // (1 << 20)),
        name="attend",
    )(q, *blocks, in_hbm(w_out))


def combine(own, gate, got, mine):
    share, model = own.shape
    chunks = len(got)
    cw = model // chunks

    def kernel(own_ref, gate_ref, *refs):
        gs, ms, out = refs[:chunks], refs[chunks : 2 * chunks], refs[2 * chunks]
        first = pl.multiple_of(lax.axis_index("tp") * share, share)
        g = gate_ref[pl.ds(first, share), 0:1]
        for i in range(chunks):
            at = slice(i * cw, (i + 1) * cw)
            proj = gs[i][...].astype(F32) + ms[i][...]
            out[:, at] = (own_ref[:, at].astype(F32) + g * proj).astype(BF)

    return pl.pallas_call(
        kernel,
        out_shape=sds((share, model), BF),
        in_specs=[VMEM] * (2 + 2 * chunks),
        out_specs=VMEM,
        cost_estimate=cost(1 << 20, 8 * share * model),
        compiler_params=params(8),
        name="combine",
    )(own, gate, *got, *mine)


def on_device(resid, sel_blocks, norm_gain, router_weight, w_query, w_key, value_projection, w_out):
    picked = sel_blocks.shape[0]
    n = lax.axis_size("tp")
    spans = lax.axis_size("ctx")
    rows = picked * BLK
    share = rows // n
    weights = (w_query, w_key, value_projection)
    up = [(i, (i + 1) % n) for i in range(n)]
    down = [(i, (i - 1) % n) for i in range(n)]
    ways = [up, down] * GATHER_WAYS

    positions = (sel_blocks[:, None] * BLK + jnp.arange(BLK, dtype=jnp.int32)[None, :]).reshape(rows)
    half = HEAD_WIDTH // 2
    freqs = jnp.exp(jnp.arange(half, dtype=F32) * (-2.0 * math.log(rope_base) / HEAD_WIDTH))
    angles = positions.astype(F32)[:, None] * freqs[None, :]
    cos, sin = jnp.cos(angles), jnp.sin(angles)
    cos2 = jnp.concatenate([cos, cos], axis=1)
    sin2 = jnp.concatenate([-sin, sin], axis=1)
    gain = norm_gain.reshape(1, -1)
    router = router_weight.reshape(1, -1)

    held = pick_rows(resid, sel_blocks, len(ways))
    state = None
    for s in range(n - 1):
        moved = [lax.ppermute(b, "tp", way) for b, way in zip(held, ways)]
        state = accumulate(s, n, held, gain, router, weights, state, share)
        if s < n - 2:
            moved, tied = lax.optimization_barrier((moved, state[3]))
            state = [*state[:3], tied, *state[4:]]
        held = moved
    last = held
    kv, inv, gate = finish_kv(n - 1, n, last, gain, router, weights, state, cos2, sin2)

    blocks = [None] * spans
    blocks[0] = kv
    for k in range(2, spans, 2):
        blocks[k] = lax.ppermute(kv, "ctx", [(i, i ^ k) for i in range(spans)])
    for k in range(0, spans, 2):
        blocks[k + 1] = lax.ppermute(blocks[k], "ctx", [(i, i ^ 1) for i in range(spans)])
    q, own = finish_q(n - 1, n, last, gain, weights, state, inv, cos2, sin2, share)

    out_ways = [up, down] * SCATTER_WAYS
    chunks = len(out_ways)
    near = attend(
        q, blocks, w_out, share, [n - 1, 1], chunks,
        [[BF if k % 2 == d else F32 for k in range(chunks)] for d in range(2)],
    )
    rest = list(range(2, n - 1)) + [0]
    far = attend(q, blocks, w_out, share, rest, chunks, [[F32] * chunks] * len(rest))
    parts = {}
    for d, off in enumerate([n - 1, 1]):
        parts[off] = near[d * chunks : (d + 1) * chunks]
    for d, off in enumerate(rest):
        parts[off] = far[d * chunks : (d + 1) * chunks]

    moving = [parts[n - 1 if k % 2 == 0 else 1][k] for k in range(chunks)]
    for s in range(1, n):
        moving = [lax.ppermute(b, "tp", way) for b, way in zip(moving, out_ways)]
        if s < n - 1:
            moving = [
                (b.astype(F32) + parts[(n - 1 - s if k % 2 == 0 else 1 + s)][k]).astype(BF)
                for k, b in enumerate(moving)
            ]
    return combine(own, gate, moving, parts[0])


def solution(mesh):
    return jax.shard_map(
        on_device,
        mesh=mesh,
        in_specs=(
            P("ctx", "tp"),
            P("ctx"),
            P(),
            P(),
            P(None, "tp"),
            P(None, "tp"),
            P(None, "tp"),
            P("tp", None),
        ),
        out_specs=P(("ctx", "tp"), None),
        check_vma=False,
    )
```

```python
import math

import jax
import jax.numpy as jnp
from jax import lax
from jax.experimental import pallas as pl
from jax.experimental.pallas import tpu as pltpu
from jax.sharding import PartitionSpec as P

HEAD_WIDTH = 128
BLK = 128

rope_base = 500000.0
norm_eps = 1e-05
score_scale = math.log2(math.e) / math.sqrt(HEAD_WIDTH)

GATHER_WAYS = 1
SCATTER_WAYS = 1


VMEM = pl.BlockSpec(memory_space=pltpu.VMEM)
SMEM = pl.BlockSpec(memory_space=pltpu.SMEM)
HBM = pl.BlockSpec(memory_space=pltpu.HBM)
BF = jnp.bfloat16
F32 = jnp.float32


def sds(shape, dtype):
    return jax.ShapeDtypeStruct(shape, dtype)


def cost(flops, nbytes):
    return pl.CostEstimate(flops=int(flops), bytes_accessed=int(nbytes), transcendentals=0)


def in_hbm(x):
    return pltpu.with_memory_space_constraint(x, pltpu.HBM)


def params(mib):
    return pltpu.CompilerParams(vmem_limit_bytes=mib << 20)


def pick_rows(resid, sel_blocks, pieces):
    local_rows, width = resid.shape
    w = width // pieces
    picked = sel_blocks.shape[0]
    block_count = local_rows // BLK

    def kernel(sel, x_hbm, *refs):
        outs, sems = refs[:pieces], refs[pieces]
        copies = []
        for i in range(picked):
            at = pl.ds(pl.multiple_of(lax.rem(sel[i], block_count) * BLK, BLK), BLK)
            for p in range(pieces):
                copies.append(
                    pltpu.make_async_copy(
                        x_hbm.at[at, p * w : (p + 1) * w],
                        outs[p].at[i * BLK : (i + 1) * BLK, :],
                        sems.at[i, p],
                    )
                )
        for c in copies:
            c.start()
        for c in copies:
            c.wait()

    return pl.pallas_call(
        kernel,
        out_shape=[sds((picked * BLK, w), BF)] * pieces,
        in_specs=[SMEM, HBM],
        out_specs=[VMEM] * pieces,
        scratch_shapes=[pltpu.SemaphoreType.DMA((picked, pieces))],
        cost_estimate=cost(1 << 20, 4 * picked * BLK * width),
        compiler_params=params(8),
        name="pick",
    )(in_hbm(sel_blocks), in_hbm(resid))


def stage_weights(after, arrays):
    count = len(arrays)

    def kernel(*refs):
        ins, outs, sems = refs[1 : 1 + count], refs[1 + count : 1 + 2 * count], refs[1 + 2 * count]
        copies = [
            pltpu.make_async_copy(a, b, sems.at[i]) for i, (a, b) in enumerate(zip(ins, outs))
        ]
        for c in copies:
            c.start()
        for c in copies:
            c.wait()

    return pl.pallas_call(
        kernel,
        out_shape=[sds(a.shape, a.dtype) for a in arrays],
        in_specs=[pl.BlockSpec(memory_space=pl.ANY)] + [HBM] * count,
        out_specs=[VMEM] * count,
        scratch_shapes=[pltpu.SemaphoreType.DMA((count,))],
        cost_estimate=cost(1 << 30, sum(a.size * a.dtype.itemsize for a in arrays)),
        compiler_params=params(4),
        name="stage_weights",
    )(after, *map(in_hbm, arrays))


def rotate_half(x, cos2, sin2):
    return x * cos2 + pltpu.roll(x, HEAD_WIDTH // 2, 1) * sin2


def ring_of(n):
    return list(range(0, 1)) + list(range(1, n, 2)) + list(range(2, n, 2))[::-1]


def look_up(table, index):
    out = jnp.int32(table[0])
    for i, value in enumerate(table[1:], 1):
        out = jnp.where(index == i, jnp.int32(value), out)
    return out


def at_offset(offset, n):
    ring = ring_of(n)
    place = look_up([ring.index(i) for i in range(n)], lax.axis_index("tp"))
    return look_up(ring, lax.rem(place + offset % n, n))


def piece_index(stage, k, n, chains):
    return at_offset(-stage if k % 2 == 0 else stage, n) * chains + k


def gained(x, at, gain_ref):
    return (x.astype(F32) * gain_ref[:, at]).astype(BF)


def accumulate(stage, n, pieces, gain, router, weights, state, share):
    count = len(pieces)
    rows, w = pieces[0].shape
    wq, wk, wv = weights
    nq, nk = wq.shape[1], wk.shape[1]
    features = gain.shape[1]
    held = 0 if state is None else len(state)

    def kernel(*refs):
        xs = refs[:count]
        gain_ref, router_ref, wqr, wkr, wvr = refs[count : count + 5]
        before = refs[count + 5 : count + 5 + held]
        q_out, k_out, v_out, ss_out, gd_out, own_out = refs[count + 5 + held :]
        offsets = [
            pl.multiple_of(piece_index(stage, p, n, count) * w, w) for p in range(count)
        ]
        first = pl.multiple_of(lax.axis_index("tp") * share, share)
        xg = []
        ss = gd = None
        for p in range(count):
            at = pl.ds(offsets[p], w)
            x = xs[p][...].astype(F32)
            a = jnp.sum(x * x, axis=1, keepdims=True)
            b = jnp.sum(x * router_ref[:, at], axis=1, keepdims=True)
            ss = a if ss is None else ss + a
            gd = b if gd is None else gd + b
            xg.append((x * gain_ref[:, at]).astype(BF))
            own_out[:, at] = xs[p][pl.ds(first, share), :]
        for ref, out, weight in ((0, q_out, wqr), (1, k_out, wkr), (2, v_out, wvr)):
            total = before[ref][...] if held else None
            for p in range(count):
                d = jnp.dot(xg[p], weight[pl.ds(offsets[p], w), :], preferred_element_type=F32)
                total = d if total is None else total + d
            out[...] = total
        ss_out[...] = ss + before[3][...] if held else ss
        gd_out[...] = gd + before[4][...] if held else gd

    shapes = [
        sds((rows, nq), F32),
        sds((rows, nk), F32),
        sds((rows, nk), F32),
        sds((rows, 1), F32),
        sds((rows, 1), F32),
        sds((share, features), BF),
    ]
    return pl.pallas_call(
        kernel,
        out_shape=shapes,
        in_specs=[VMEM] * (count + 5 + held),
        out_specs=[VMEM] * 6,
        input_output_aliases={count + 5 + i: i for i in range(held)},
        cost_estimate=cost(2 * rows * w * count * (nq + 2 * nk), 2 * count * w * (nq + 2 * nk)),
        compiler_params=params(16),
        name="accumulate",
    )(*pieces, gain, router, *weights, *(state or ()))


def finish_kv(stage, n, pieces, gain, router, weights, state, cos2, sin2):
    count = len(pieces)
    rows, w = pieces[0].shape
    wq, wk, wv = weights
    nk = wk.shape[1]
    features = gain.shape[1]

    def kernel(*refs):
        xs = refs[:count]
        gain_ref, router_ref, wkr, wvr, ka, va, ssa, gda, cos_ref, sin_ref = refs[
            count : count + 10
        ]
        kv_out, inv_out, gate_out = refs[count + 10 :]
        offsets = [
            pl.multiple_of(piece_index(stage, p, n, count) * w, w) for p in range(count)
        ]
        ss, gd = ssa[...], gda[...]
        xg = []
        for p in range(count):
            at = pl.ds(offsets[p], w)
            x = xs[p][...].astype(F32)
            ss += jnp.sum(x * x, axis=1, keepdims=True)
            gd += jnp.sum(x * router_ref[:, at], axis=1, keepdims=True)
            xg.append((x * gain_ref[:, at]).astype(BF))
        inv = jnp.broadcast_to(lax.rsqrt(ss * (1.0 / features) + norm_eps), (rows, HEAD_WIDTH))
        inv_out[...] = inv
        gate_out[...] = jnp.broadcast_to(1.0 / (1.0 + jnp.exp(-gd)), gate_out.shape)
        k, v = ka[...], va[...]
        for p in range(count):
            at = pl.ds(offsets[p], w)
            k += jnp.dot(xg[p], wkr[at, :], preferred_element_type=F32)
            v += jnp.dot(xg[p], wvr[at, :], preferred_element_type=F32)
        cos, sin = cos_ref[...] * inv, sin_ref[...] * inv
        for h in range(nk // HEAD_WIDTH):
            at = slice(h * HEAD_WIDTH, (h + 1) * HEAD_WIDTH)
            to = slice(nk + h * HEAD_WIDTH, nk + (h + 1) * HEAD_WIDTH)
            kv_out[:, at] = rotate_half(k[:, at], cos, sin).astype(BF)
            kv_out[:, to] = (v[:, at] * inv).astype(BF)

    return pl.pallas_call(
        kernel,
        out_shape=[
            sds((rows, 2 * nk), BF),
            sds((rows, HEAD_WIDTH), F32),
            sds((rows, HEAD_WIDTH), F32),
        ],
        in_specs=[VMEM] * (count + 10),
        out_specs=[VMEM] * 3,
        cost_estimate=cost(4 * rows * w * count * nk, 4 * count * w * nk),
        compiler_params=params(8),
        name="finish_kv",
    )(*pieces, gain, router, wk, wv, state[1], state[2], state[3], state[4], cos2, sin2)


def finish_q(stage, n, pieces, gain, weights, state, inv, cos2, sin2, share):
    count = len(pieces)
    rows, w = pieces[0].shape
    wq = weights[0]
    nq = wq.shape[1]
    features = gain.shape[1]

    def kernel(*refs):
        xs = refs[:count]
        gain_ref, wqr, qa, own_in, inv_ref, cos_ref, sin_ref = refs[count : count + 7]
        q_out, own_out = refs[count + 7 :]
        offsets = [
            pl.multiple_of(piece_index(stage, p, n, count) * w, w) for p in range(count)
        ]
        first = pl.multiple_of(lax.axis_index("tp") * share, share)
        xg = []
        for p in range(count):
            at = pl.ds(offsets[p], w)
            xg.append((xs[p][...].astype(F32) * gain_ref[:, at]).astype(BF))
            own_out[:, at] = xs[p][pl.ds(first, share), :]
        factor = inv_ref[...] * score_scale
        cos, sin = cos_ref[...] * factor, sin_ref[...] * factor
        for h in range(0, nq, 2 * HEAD_WIDTH):
            both = slice(h, h + 2 * HEAD_WIDTH)
            q = qa[:, both]
            for p in range(count):
                q += jnp.dot(
                    xg[p], wqr[pl.ds(offsets[p], w), both], preferred_element_type=F32
                )
            for i in range(2):
                at = slice(i * HEAD_WIDTH, (i + 1) * HEAD_WIDTH)
                to = slice(h + i * HEAD_WIDTH, h + (i + 1) * HEAD_WIDTH)
                q_out[:, to] = rotate_half(q[:, at], cos, sin).astype(BF)

    return pl.pallas_call(
        kernel,
        out_shape=[sds((rows, nq), BF), sds((share, features), BF)],
        in_specs=[VMEM] * (count + 7),
        out_specs=[VMEM] * 2,
        input_output_aliases={count + 3: 1},
        cost_estimate=cost(2 * rows * w * count * nq, 2 * count * w * nq),
        compiler_params=params(12),
        name="finish_q",
    )(*pieces, gain, wq, state[0], state[5], inv, cos2, sin2)


def attend(q, blocks, w_out, share, segments, dtypes):
    n = lax.axis_size("tp")
    rows, nq = q.shape
    heads = nq // HEAD_WIDTH
    nk = blocks[0].shape[1] // 2
    kv_heads = nk // HEAD_WIDTH
    group = heads // kv_heads
    sizes = [seg[2] for seg in segments]
    bases = [sum(sizes[:i]) for i in range(len(sizes))]
    part = sum(sizes)
    spans = len(blocks)
    taken = group
    while taken % 2 == 0 and spans * rows * taken * part * 4 > 16 << 20:
        taken //= 2
    tall = taken * part
    model = w_out.shape[1]
    cw = 1024 if model % 1024 == 0 else model
    count = len(segments)
    groups = []
    bit = 1
    while bit < spans:
        for k in range(bit, 2 * bit, 4):
            groups.append((bit, range(k, min(k + 4, 2 * bit))))
        bit *= 2

    def kernel(*refs):
        q_ref = refs[0]
        kvs = refs[1 : 1 + spans]
        w_ref = refs[1 + spans]
        outs = refs[2 + spans : 2 + spans + count]
        qs, vs, sc, m_ref, acc, att = refs[2 + spans + count :]
        me = lax.axis_index("ctx")
        starts = [
            pl.multiple_of(at_offset(off, n) * share + lo, math.gcd(share, lo) if lo else share)
            for off, lo, size in segments
        ]
        for k in range(spans):
            vs[k, :, HEAD_WIDTH:] = jnp.ones((rows, HEAD_WIDTH), BF)
        for base in range(0, heads, taken):
            kh = base // group
            for h in range(taken):
                col = (base + h) * HEAD_WIDTH
                for d in range(count):
                    to = h * part + bases[d]
                    qs[to : to + sizes[d], :] = q_ref[
                        pl.ds(starts[d], sizes[d]), col : col + HEAD_WIDTH
                    ]
            k_at = slice(kh * HEAD_WIDTH, (kh + 1) * HEAD_WIDTH)
            v_at = slice(nk + kh * HEAD_WIDTH, nk + (kh + 1) * HEAD_WIDTH)

            def score(k):
                return lax.dot_general(
                    qs[...],
                    kvs[k][:, k_at],
                    (((1,), (1,)), ((), ())),
                    preferred_element_type=F32,
                )

            def top(m, s):
                for i in range(rows // HEAD_WIDTH):
                    m = jnp.maximum(m, s[:, i * HEAD_WIDTH : (i + 1) * HEAD_WIDTH])
                return m

            def scores_of(span_group):
                m = m_ref[...]
                for k in span_group:
                    s = score(k)
                    sc[k] = s
                    m = top(m, s)
                m_ref[...] = m

            def weigh(span_group):
                m = m_ref[...]
                total = None
                for k in span_group:
                    vs[k, :, :HEAD_WIDTH] = kvs[k][:, v_at]
                    p = jnp.concatenate(
                        [
                            jnp.exp2(sc[k, :, i * HEAD_WIDTH : (i + 1) * HEAD_WIDTH] - m).astype(BF)
                            for i in range(rows // HEAD_WIDTH)
                        ],
                        axis=1,
                    )
                    d = jnp.dot(p, vs[k], preferred_element_type=F32)
                    total = d if total is None else total + d
                return total

            own_rows = jnp.concatenate(
                [lax.broadcasted_iota(jnp.int32, (size, 1), 0) + s for s, size in zip(starts, sizes)]
                * taken,
                axis=0,
            )
            key = lax.broadcasted_iota(jnp.int32, (tall, rows), 1)
            s = jnp.where(key <= own_rows, score(0), -1e30)
            sc[0] = s
            m_ref[...] = top(s[:, :HEAD_WIDTH], s)
            for bit, span_group in groups:

                @pl.when((me & bit) != 0)
                def _():
                    scores_of(span_group)

            m_ref[...] = jnp.broadcast_to(
                jnp.max(m_ref[...], axis=1, keepdims=True), m_ref.shape
            )
            acc[...] = weigh([0])
            for bit, span_group in groups:

                @pl.when((me & bit) != 0)
                def _():
                    acc[...] += weigh(span_group)

            done = (acc[:, :HEAD_WIDTH] / acc[:, HEAD_WIDTH:]).astype(BF)
            for h in range(taken):
                col = (base + h) * HEAD_WIDTH
                att[:, col : col + HEAD_WIDTH] = done[h * part : (h + 1) * part, :]
        for i in range(model // cw):
            at = slice(i * cw, (i + 1) * cw)
            proj = jnp.dot(att[...], w_ref[:, at], preferred_element_type=F32)
            for d in range(count):
                piece = proj[bases[d] : bases[d] + sizes[d], :]
                outs[d][:, at] = piece.astype(outs[d].dtype)

    return pl.pallas_call(
        kernel,
        out_shape=[sds((size, model), dt) for size, dt in zip(sizes, dtypes)],
        in_specs=[VMEM] * (2 + spans),
        out_specs=[VMEM] * count,
        scratch_shapes=[
            pltpu.VMEM((tall, HEAD_WIDTH), BF),
            pltpu.VMEM((spans, rows, 2 * HEAD_WIDTH), BF),
            pltpu.VMEM((spans, tall, rows), F32),
            pltpu.VMEM((tall, HEAD_WIDTH), F32),
            pltpu.VMEM((tall, 2 * HEAD_WIDTH), F32),
            pltpu.VMEM((part, nq), BF),
        ],
        cost_estimate=cost(
            4 * part * nq * rows * spans + 2 * part * nq * model,
            2 * nq * model + 2 * spans * rows * nk,
        ),
        compiler_params=params(10 + spans * tall * rows * 4 // (1 << 20)),
        name="attend",
    )(q, *blocks, w_out)


def combine(own, gate, got, mine):
    share, model = own.shape
    count = len(got)
    size = share // count

    def kernel(own_ref, gate_ref, mine_ref, *refs):
        gs, out = refs[:count], refs[count]
        first = pl.multiple_of(lax.axis_index("tp") * share, share)
        g = gate_ref[pl.ds(first, share), 0:1]
        for i in range(count):
            at = slice(i * size, (i + 1) * size)
            proj = gs[i][...].astype(F32) + mine_ref[at, :]
            out[at, :] = (own_ref[at, :].astype(F32) + g[at, :] * proj).astype(BF)

    return pl.pallas_call(
        kernel,
        out_shape=sds((share, model), BF),
        in_specs=[VMEM] * (3 + count),
        out_specs=VMEM,
        cost_estimate=cost(1 << 20, 8 * share * model),
        compiler_params=params(8),
        name="combine",
    )(own, gate, mine, *got)


def on_device(resid, sel_blocks, norm_gain, router_weight, w_query, w_key, value_projection, w_out):
    picked = sel_blocks.shape[0]
    n = lax.axis_size("tp")
    spans = lax.axis_size("ctx")
    rows = picked * BLK
    share = rows // n
    weights = (w_query, w_key, value_projection)
    ring = ring_of(n)
    up = [(ring[i], ring[(i + 1) % n]) for i in range(n)]
    down = [(ring[i], ring[i - 1]) for i in range(n)]
    ways = [up, down] * GATHER_WAYS

    positions = (sel_blocks[:, None] * BLK + jnp.arange(BLK, dtype=jnp.int32)[None, :]).reshape(rows)
    half = HEAD_WIDTH // 2
    freqs = jnp.exp(jnp.arange(half, dtype=F32) * (-2.0 * math.log(rope_base) / HEAD_WIDTH))
    angles = positions.astype(F32)[:, None] * freqs[None, :]
    cos, sin = jnp.cos(angles), jnp.sin(angles)
    cos2 = jnp.concatenate([cos, cos], axis=1)
    sin2 = jnp.concatenate([-sin, sin], axis=1)
    gain = norm_gain.reshape(1, -1)
    router = router_weight.reshape(1, -1)

    stages = [pick_rows(resid, sel_blocks, len(ways))]
    *weights, gain, router = stage_weights(stages[0][0], [*weights, gain, router])
    tie = gain
    state = None
    for s in range(n - 1):
        held = [lax.ppermute(b, "tp", way) for b, way in zip(stages[s], ways)]
        if s:
            state = accumulate(s - 1, n, stages[s - 1], gain, router, weights, state, share)
            tie = state[3]
        if s < n - 2:
            held = [lax.optimization_barrier((b, tie))[0] for b in held]
        stages.append(held)
    state = accumulate(n - 2, n, stages[n - 2], gain, router, weights, state, share)
    last = stages[n - 1]
    kv, inv, gate = finish_kv(n - 1, n, last, gain, router, weights, state, cos2, sin2)

    blocks = [None] * spans
    blocks[0] = kv
    for k in range(2, spans, 2):
        blocks[k] = lax.ppermute(kv, "ctx", [(i, i ^ k) for i in range(spans)])
    q, own = finish_q(n - 1, n, last, gain, weights, state, inv, cos2, sin2, share)
    for k in range(0, spans, 2):
        block = blocks[k]
        if k:
            block = lax.optimization_barrier((block, own))[0]
        blocks[k + 1] = lax.ppermute(block, "ctx", [(i, i ^ 1) for i in range(spans)])

    chains = 2 * SCATTER_WAYS
    size = share // chains
    out_ways = [up, down] * SCATTER_WAYS

    def segment(step, k):
        return ((n - 1 - step) if k % 2 == 0 else 1 + step, k * size, size)

    near = attend(
        q, blocks, w_out, share, [segment(0, k) for k in range(chains)], [BF] * chains
    )
    later = [segment(s, k) for s in range(1, n - 1) for k in range(chains)]
    far = attend(
        q, blocks, w_out, share, later + [(0, 0, share)], [F32] * (len(later) + 1)
    )
    moving = near
    for s in range(1, n):
        moving = [lax.ppermute(b, "tp", way) for b, way in zip(moving, out_ways)]
        if s < n - 1:
            mine = far[(s - 1) * chains : s * chains]
            moving = [(b.astype(F32) + m).astype(BF) for b, m in zip(moving, mine)]
    return combine(own, gate, moving, far[-1])


def solution(mesh):
    return jax.shard_map(
        on_device,
        mesh=mesh,
        in_specs=(
            P("ctx", "tp"),
            P("ctx"),
            P(),
            P(),
            P(None, "tp"),
            P(None, "tp"),
            P(None, "tp"),
            P("tp", None),
        ),
        out_specs=P(("ctx", "tp"), None),
        check_vma=False,
    )
```

```python
import math

import jax
import jax.numpy as jnp
from jax import lax
from jax.experimental import pallas as pl
from jax.experimental.pallas import tpu as pltpu
from jax.sharding import PartitionSpec as P


HEAD_WIDTH = 128
BLK = 128

rope_base = 500000.0
norm_eps = 1e-05
score_scale = math.log2(math.e) / math.sqrt(HEAD_WIDTH)

GATHER_WAYS = 1
SCATTER_WAYS = 1


VMEM = pl.BlockSpec(memory_space=pltpu.VMEM)
SMEM = pl.BlockSpec(memory_space=pltpu.SMEM)
HBM = pl.BlockSpec(memory_space=pltpu.HBM)
BF = jnp.bfloat16
F32 = jnp.float32


def sds(shape, dtype):
    return jax.ShapeDtypeStruct(shape, dtype)


def cost(flops, nbytes):
    return pl.CostEstimate(flops=int(flops), bytes_accessed=int(nbytes), transcendentals=0)


def in_hbm(x):
    return pltpu.with_memory_space_constraint(x, pltpu.HBM)


def params(mib):
    return pltpu.CompilerParams(vmem_limit_bytes=mib << 20)


def pick_rows(resid, sel_blocks, pieces):
    local_rows, width = resid.shape
    w = width // pieces
    picked = sel_blocks.shape[0]
    block_count = local_rows // BLK

    def kernel(sel, x_hbm, *refs):
        outs, sems = refs[:pieces], refs[pieces]
        copies = []
        for i in range(picked):
            at = pl.ds(pl.multiple_of(lax.rem(sel[i], block_count) * BLK, BLK), BLK)
            for p in range(pieces):
                copies.append(
                    pltpu.make_async_copy(
                        x_hbm.at[at, p * w : (p + 1) * w],
                        outs[p].at[i * BLK : (i + 1) * BLK, :],
                        sems.at[i, p],
                    )
                )
        for c in copies:
            c.start()
        for c in copies:
            c.wait()

    return pl.pallas_call(
        kernel,
        out_shape=[sds((picked * BLK, w), BF)] * pieces,
        in_specs=[SMEM, HBM],
        out_specs=[VMEM] * pieces,
        scratch_shapes=[pltpu.SemaphoreType.DMA((picked, pieces))],
        cost_estimate=cost(1 << 20, 4 * picked * BLK * width),
        compiler_params=params(8),
        name="pick",
    )(in_hbm(sel_blocks), in_hbm(resid))


def stage_weights(after, arrays):
    count = len(arrays)

    def kernel(*refs):
        ins, outs, sems = refs[1 : 1 + count], refs[1 + count : 1 + 2 * count], refs[1 + 2 * count]
        copies = [
            pltpu.make_async_copy(a, b, sems.at[i]) for i, (a, b) in enumerate(zip(ins, outs))
        ]
        for c in copies:
            c.start()
        for c in copies:
            c.wait()

    return pl.pallas_call(
        kernel,
        out_shape=[sds(a.shape, a.dtype) for a in arrays],
        in_specs=[pl.BlockSpec(memory_space=pl.ANY)] + [HBM] * count,
        out_specs=[VMEM] * count,
        scratch_shapes=[pltpu.SemaphoreType.DMA((count,))],
        cost_estimate=cost(1 << 30, sum(a.size * a.dtype.itemsize for a in arrays)),
        compiler_params=params(4),
        name="stage_weights",
    )(after, *map(in_hbm, arrays))


def rotate_half(x, cos2, sin2):
    return x * cos2 + pltpu.roll(x, HEAD_WIDTH // 2, 1) * sin2


def ring_of(n):
    return list(range(0, 1)) + list(range(1, n, 2)) + list(range(2, n, 2))[::-1]


def look_up(table, index):
    out = jnp.int32(table[0])
    for i, value in enumerate(table[1:], 1):
        out = jnp.where(index == i, jnp.int32(value), out)
    return out


def at_offset(offset, n):
    ring = ring_of(n)
    place = look_up([ring.index(i) for i in range(n)], lax.axis_index("tp"))
    return look_up(ring, lax.rem(place + offset % n, n))


def piece_index(stage, k, n, chains):
    return at_offset(-stage if k % 2 == 0 else stage, n) * chains + k


def accumulate(stage, n, pieces, gain, router, weights, state, share):
    count = len(pieces)
    rows, w = pieces[0].shape
    wq, wk, _ = weights
    nq, nk = wq.shape[1], wk.shape[1]
    features = gain.shape[1]
    held = 0 if state is None else len(state)

    def kernel(*refs):
        xs = refs[:count]
        gain_ref, router_ref, wqr, wkr, wvr = refs[count : count + 5]
        before = refs[count + 5 : count + 5 + held]
        q_out, k_out, v_out, ss_out, gd_out, own_out = refs[count + 5 + held :]
        offsets = [
            pl.multiple_of(piece_index(stage, p, n, count) * w, w) for p in range(count)
        ]
        first = pl.multiple_of(lax.axis_index("tp") * share, share)
        xg = []
        ss = gd = None
        for p in range(count):
            at = pl.ds(offsets[p], w)
            x = xs[p][...].astype(F32)
            a = jnp.sum(x * x, axis=1, keepdims=True)
            b = jnp.sum(x * router_ref[:, at], axis=1, keepdims=True)
            ss = a if ss is None else ss + a
            gd = b if gd is None else gd + b
            xg.append((x * gain_ref[:, at]).astype(BF))
            own_out[:, at] = xs[p][pl.ds(first, share), :]
        for ref, out, weight in ((0, q_out, wqr), (1, k_out, wkr), (2, v_out, wvr)):
            total = before[ref][...] if held else None
            for p in range(count):
                d = jnp.dot(xg[p], weight[pl.ds(offsets[p], w), :], preferred_element_type=F32)
                total = d if total is None else total + d
            out[...] = total
        ss_out[...] = ss + before[3][...] if held else ss
        gd_out[...] = gd + before[4][...] if held else gd

    shapes = [
        sds((rows, nq), F32),
        sds((rows, nk), F32),
        sds((rows, nk), F32),
        sds((rows, 1), F32),
        sds((rows, 1), F32),
        sds((share, features), BF),
    ]
    return pl.pallas_call(
        kernel,
        out_shape=shapes,
        in_specs=[VMEM] * (count + 5 + held),
        out_specs=[VMEM] * 6,
        input_output_aliases={count + 5 + i: i for i in range(held)},
        cost_estimate=cost(2 * rows * w * count * (nq + 2 * nk), 2 * count * w * (nq + 2 * nk)),
        compiler_params=params(16),
        name="accumulate",
    )(*pieces, gain, router, *weights, *(state or ()))


def finish_kv(stage, n, pieces, gain, router, weights, state, cos2, sin2):
    count = len(pieces)
    rows, w = pieces[0].shape
    _, wk, wv = weights
    nk = wk.shape[1]
    features = gain.shape[1]

    def kernel(*refs):
        xs = refs[:count]
        gain_ref, router_ref, wkr, wvr, ka, va, ssa, gda, cos_ref, sin_ref = refs[
            count : count + 10
        ]
        kv_out, inv_out, gate_out = refs[count + 10 :]
        offsets = [
            pl.multiple_of(piece_index(stage, p, n, count) * w, w) for p in range(count)
        ]
        ss, gd = ssa[...], gda[...]
        xg = []
        for p in range(count):
            at = pl.ds(offsets[p], w)
            x = xs[p][...].astype(F32)
            ss += jnp.sum(x * x, axis=1, keepdims=True)
            gd += jnp.sum(x * router_ref[:, at], axis=1, keepdims=True)
            xg.append((x * gain_ref[:, at]).astype(BF))
        inv = jnp.broadcast_to(lax.rsqrt(ss * (1.0 / features) + norm_eps), (rows, HEAD_WIDTH))
        inv_out[...] = inv
        gate_out[...] = jnp.broadcast_to(1.0 / (1.0 + jnp.exp(-gd)), gate_out.shape)
        k, v = ka[...], va[...]
        for p in range(count):
            at = pl.ds(offsets[p], w)
            k += jnp.dot(xg[p], wkr[at, :], preferred_element_type=F32)
            v += jnp.dot(xg[p], wvr[at, :], preferred_element_type=F32)
        cos, sin = cos_ref[...] * inv, sin_ref[...] * inv
        for h in range(nk // HEAD_WIDTH):
            at = slice(h * HEAD_WIDTH, (h + 1) * HEAD_WIDTH)
            to = slice(nk + h * HEAD_WIDTH, nk + (h + 1) * HEAD_WIDTH)
            kv_out[:, at] = rotate_half(k[:, at], cos, sin).astype(BF)
            kv_out[:, to] = (v[:, at] * inv).astype(BF)

    return pl.pallas_call(
        kernel,
        out_shape=[
            sds((rows, 2 * nk), BF),
            sds((rows, HEAD_WIDTH), F32),
            sds((rows, HEAD_WIDTH), F32),
        ],
        in_specs=[VMEM] * (count + 10),
        out_specs=[VMEM] * 3,
        cost_estimate=cost(4 * rows * w * count * nk, 4 * count * w * nk),
        compiler_params=params(8),
        name="finish_kv",
    )(*pieces, gain, router, wk, wv, state[1], state[2], state[3], state[4], cos2, sin2)


def finish_q(stage, n, pieces, gain, weights, state, inv, cos2, sin2, share):
    count = len(pieces)
    rows, w = pieces[0].shape
    wq = weights[0]
    nq = wq.shape[1]
    features = gain.shape[1]

    def kernel(*refs):
        xs = refs[:count]
        gain_ref, wqr, qa, _, inv_ref, cos_ref, sin_ref = refs[count : count + 7]
        q_out, own_out = refs[count + 7 :]
        offsets = [
            pl.multiple_of(piece_index(stage, p, n, count) * w, w) for p in range(count)
        ]
        first = pl.multiple_of(lax.axis_index("tp") * share, share)
        xg = []
        for p in range(count):
            at = pl.ds(offsets[p], w)
            xg.append((xs[p][...].astype(F32) * gain_ref[:, at]).astype(BF))
            own_out[:, at] = xs[p][pl.ds(first, share), :]
        factor = inv_ref[...] * score_scale
        cos, sin = cos_ref[...] * factor, sin_ref[...] * factor
        for h in range(0, nq, 2 * HEAD_WIDTH):
            both = slice(h, h + 2 * HEAD_WIDTH)
            q = qa[:, both]
            for p in range(count):
                q += jnp.dot(
                    xg[p], wqr[pl.ds(offsets[p], w), both], preferred_element_type=F32
                )
            for i in range(2):
                at = slice(i * HEAD_WIDTH, (i + 1) * HEAD_WIDTH)
                to = slice(h + i * HEAD_WIDTH, h + (i + 1) * HEAD_WIDTH)
                q_out[:, to] = rotate_half(q[:, at], cos, sin).astype(BF)

    return pl.pallas_call(
        kernel,
        out_shape=[sds((rows, nq), BF), sds((share, features), BF)],
        in_specs=[VMEM] * (count + 7),
        out_specs=[VMEM] * 2,
        input_output_aliases={count + 3: 1},
        cost_estimate=cost(2 * rows * w * count * nq, 2 * count * w * nq),
        compiler_params=params(12),
        name="finish_q",
    )(*pieces, gain, wq, state[0], state[5], inv, cos2, sin2)


def attend(q, blocks, w_out, share, segments, dtypes):
    n = lax.axis_size("tp")
    rows, nq = q.shape
    heads = nq // HEAD_WIDTH
    nk = blocks[0].shape[1] // 2
    kv_heads = nk // HEAD_WIDTH
    group = heads // kv_heads
    sizes = [seg[2] for seg in segments]
    bases = [sum(sizes[:i]) for i in range(len(sizes))]
    part = sum(sizes)
    spans = len(blocks)
    taken = group
    while taken % 2 == 0 and spans * rows * taken * part * 4 > 16 << 20:
        taken //= 2
    tall = taken * part
    model = w_out.shape[1]
    cw = 1024 if model % 1024 == 0 else model
    count = len(segments)
    groups = []
    bit = 1
    while bit < spans:
        for k in range(bit, 2 * bit, 4):
            groups.append((bit, range(k, min(k + 4, 2 * bit))))
        bit *= 2

    def kernel(*refs):
        q_ref = refs[0]
        kvs = refs[1 : 1 + spans]
        w_ref = refs[1 + spans]
        outs = refs[2 + spans : 2 + spans + count]
        qs, vs, sc, m_ref, acc, att = refs[2 + spans + count :]
        me = lax.axis_index("ctx")
        starts = [
            pl.multiple_of(at_offset(off, n) * share + lo, math.gcd(share, lo) if lo else share)
            for off, lo, size in segments
        ]
        for k in range(spans):
            vs[k, :, HEAD_WIDTH:] = jnp.ones((rows, HEAD_WIDTH), BF)
        for base in range(0, heads, taken):
            kh = base // group
            for h in range(taken):
                col = (base + h) * HEAD_WIDTH
                for d in range(count):
                    to = h * part + bases[d]
                    qs[to : to + sizes[d], :] = q_ref[
                        pl.ds(starts[d], sizes[d]), col : col + HEAD_WIDTH
                    ]
            k_at = slice(kh * HEAD_WIDTH, (kh + 1) * HEAD_WIDTH)
            v_at = slice(nk + kh * HEAD_WIDTH, nk + (kh + 1) * HEAD_WIDTH)

            def score(k):
                return lax.dot_general(
                    qs[...],
                    kvs[k][:, k_at],
                    (((1,), (1,)), ((), ())),
                    preferred_element_type=F32,
                )

            def top(m, s):
                for i in range(rows // HEAD_WIDTH):
                    m = jnp.maximum(m, s[:, i * HEAD_WIDTH : (i + 1) * HEAD_WIDTH])
                return m

            def scores_of(span_group):
                m = m_ref[...]
                for k in span_group:
                    s = score(k)
                    sc[k] = s
                    m = top(m, s)
                m_ref[...] = m

            def weigh(span_group):
                m = m_ref[...]
                total = None
                for k in span_group:
                    vs[k, :, :HEAD_WIDTH] = kvs[k][:, v_at]
                    p = jnp.concatenate(
                        [
                            jnp.exp2(sc[k, :, i * HEAD_WIDTH : (i + 1) * HEAD_WIDTH] - m).astype(BF)
                            for i in range(rows // HEAD_WIDTH)
                        ],
                        axis=1,
                    )
                    d = jnp.dot(p, vs[k], preferred_element_type=F32)
                    total = d if total is None else total + d
                return total

            own_rows = jnp.concatenate(
                [lax.broadcasted_iota(jnp.int32, (size, 1), 0) + s for s, size in zip(starts, sizes)]
                * taken,
                axis=0,
            )
            key = lax.broadcasted_iota(jnp.int32, (tall, rows), 1)
            s = jnp.where(key <= own_rows, score(0), -1e30)
            sc[0] = s
            m_ref[...] = top(s[:, :HEAD_WIDTH], s)
            for bit, span_group in groups:

                @pl.when((me & bit) != 0)
                def _():
                    scores_of(span_group)

            m_ref[...] = jnp.broadcast_to(
                jnp.max(m_ref[...], axis=1, keepdims=True), m_ref.shape
            )
            acc[...] = weigh([0])
            for bit, span_group in groups:

                @pl.when((me & bit) != 0)
                def _():
                    acc[...] += weigh(span_group)

            done = (acc[:, :HEAD_WIDTH] / acc[:, HEAD_WIDTH:]).astype(BF)
            for h in range(taken):
                col = (base + h) * HEAD_WIDTH
                att[:, col : col + HEAD_WIDTH] = done[h * part : (h + 1) * part, :]
        for i in range(model // cw):
            at = slice(i * cw, (i + 1) * cw)
            proj = jnp.dot(att[...], w_ref[:, at], preferred_element_type=F32)
            for d in range(count):
                piece = proj[bases[d] : bases[d] + sizes[d], :]
                outs[d][:, at] = piece.astype(outs[d].dtype)

    return pl.pallas_call(
        kernel,
        out_shape=[sds((size, model), dt) for size, dt in zip(sizes, dtypes)],
        in_specs=[VMEM] * (2 + spans),
        out_specs=[VMEM] * count,
        scratch_shapes=[
            pltpu.VMEM((tall, HEAD_WIDTH), BF),
            pltpu.VMEM((spans, rows, 2 * HEAD_WIDTH), BF),
            pltpu.VMEM((spans, tall, rows), F32),
            pltpu.VMEM((tall, HEAD_WIDTH), F32),
            pltpu.VMEM((tall, 2 * HEAD_WIDTH), F32),
            pltpu.VMEM((part, nq), BF),
        ],
        cost_estimate=cost(
            4 * part * nq * rows * spans + 2 * part * nq * model,
            2 * nq * model + 2 * spans * rows * nk,
        ),
        compiler_params=params(10 + spans * tall * rows * 4 // (1 << 20)),
        name="attend",
    )(q, *blocks, w_out)


def combine(own, gate, got, mine):
    share, model = own.shape
    count = len(got)
    size = share // count

    def kernel(own_ref, gate_ref, mine_ref, *refs):
        gs, out = refs[:count], refs[count]
        first = pl.multiple_of(lax.axis_index("tp") * share, share)
        g = gate_ref[pl.ds(first, share), 0:1]
        for i in range(count):
            at = slice(i * size, (i + 1) * size)
            proj = gs[i][...].astype(F32) + mine_ref[at, :]
            out[at, :] = (own_ref[at, :].astype(F32) + g[at, :] * proj).astype(BF)

    return pl.pallas_call(
        kernel,
        out_shape=sds((share, model), BF),
        in_specs=[VMEM] * (3 + count),
        out_specs=VMEM,
        cost_estimate=cost(1 << 20, 8 * share * model),
        compiler_params=params(8),
        name="combine",
    )(own, gate, mine, *got)


def on_device(resid, sel_blocks, norm_gain, router_weight, w_query, w_key, value_projection, w_out):
    picked = sel_blocks.shape[0]
    n = lax.axis_size("tp")
    spans = lax.axis_size("ctx")
    rows = picked * BLK
    share = rows // n
    weights = (w_query, w_key, value_projection)
    ring = ring_of(n)
    up = [(ring[i], ring[(i + 1) % n]) for i in range(n)]
    down = [(ring[i], ring[i - 1]) for i in range(n)]
    ways = [up, down] * GATHER_WAYS

    positions = (sel_blocks[:, None] * BLK + jnp.arange(BLK, dtype=jnp.int32)[None, :]).reshape(rows)
    half = HEAD_WIDTH // 2
    freqs = jnp.exp(jnp.arange(half, dtype=F32) * (-2.0 * math.log(rope_base) / HEAD_WIDTH))
    angles = positions.astype(F32)[:, None] * freqs[None, :]
    cos, sin = jnp.cos(angles), jnp.sin(angles)
    cos2 = jnp.concatenate([cos, cos], axis=1)
    sin2 = jnp.concatenate([-sin, sin], axis=1)
    gain = norm_gain.reshape(1, -1)
    router = router_weight.reshape(1, -1)

    stages = [pick_rows(resid, sel_blocks, len(ways))]
    *weights, gain, router = stage_weights(stages[0][0], [*weights, gain, router])
    tie = gain
    state = None
    for s in range(n - 1):
        held = [lax.ppermute(b, "tp", way) for b, way in zip(stages[s], ways)]
        if s:
            state = accumulate(s - 1, n, stages[s - 1], gain, router, weights, state, share)
            tie = state[3]
        if s < n - 2:
            held = [lax.optimization_barrier((b, tie))[0] for b in held]
        stages.append(held)
    state = accumulate(n - 2, n, stages[n - 2], gain, router, weights, state, share)
    last = stages[n - 1]
    kv, inv, gate = finish_kv(n - 1, n, last, gain, router, weights, state, cos2, sin2)

    blocks = [None] * spans
    blocks[0] = kv
    for k in range(2, spans, 2):
        blocks[k] = lax.ppermute(kv, "ctx", [(i, i ^ k) for i in range(spans)])
    q, own = finish_q(n - 1, n, last, gain, weights, state, inv, cos2, sin2, share)
    for k in range(0, spans, 2):
        block = blocks[k]
        if k:
            block = lax.optimization_barrier((block, own))[0]
        blocks[k + 1] = lax.ppermute(block, "ctx", [(i, i ^ 1) for i in range(spans)])

    chains = 2 * SCATTER_WAYS
    size = share // chains
    out_ways = [down, up] * SCATTER_WAYS

    def segment(step, k):
        return (1 + step if k % 2 == 0 else n - 1 - step, k * size, size)

    near, q_next = [], q
    for k in range(chains):
        near += attend(q_next, blocks, w_out, share, [segment(0, k)], [BF])
        q_next = lax.optimization_barrier((q, near[-1]))[0]
    later = [segment(s, k) for s in range(1, n - 1) for k in range(chains)]
    far = attend(q_next, blocks, w_out, share, later + [(0, 0, share)], [F32] * (len(later) + 1))
    moving = near
    for s in range(1, n):
        for k, way in enumerate(out_ways):
            moving[k] = lax.ppermute(moving[k], "tp", way)
        if s < n - 1:
            mine = far[(s - 1) * chains : s * chains]
            for k in range(chains):
                moving[k] = (moving[k].astype(F32) + mine[k]).astype(BF)
    return combine(own, gate, moving, far[-1])


def solution(mesh):
    return jax.shard_map(
        on_device,
        mesh=mesh,
        in_specs=(
            P("ctx", "tp"),
            P("ctx"),
            P(),
            P(),
            P(None, "tp"),
            P(None, "tp"),
            P(None, "tp"),
            P("tp", None),
        ),
        out_specs=P(("ctx", "tp"), None),
        check_vma=False,
    )
```

```python
import math

import jax
import jax.numpy as jnp
from jax import lax
from jax.experimental import pallas as pl
from jax.experimental.pallas import tpu as pltpu
from jax.sharding import PartitionSpec as P


HEAD_WIDTH = 128
BLK = 128

rope_base = 500000.0
norm_eps = 1e-05
score_scale = math.log2(math.e) / math.sqrt(HEAD_WIDTH)

GATHER_WAYS = 1
SCATTER_WAYS = 1


VMEM = pl.BlockSpec(memory_space=pltpu.VMEM)
SMEM = pl.BlockSpec(memory_space=pltpu.SMEM)
HBM = pl.BlockSpec(memory_space=pltpu.HBM)
BF = jnp.bfloat16
F32 = jnp.float32


def sds(shape, dtype):
    return jax.ShapeDtypeStruct(shape, dtype)


def cost(flops, nbytes):
    return pl.CostEstimate(flops=int(flops), bytes_accessed=int(nbytes), transcendentals=0)


def in_hbm(x):
    return pltpu.with_memory_space_constraint(x, pltpu.HBM)


def params(mib):
    return pltpu.CompilerParams(vmem_limit_bytes=mib << 20)


def pick_rows(resid, sel_blocks, pieces):
    local_rows, width = resid.shape
    w = width // pieces
    picked = sel_blocks.shape[0]
    block_count = local_rows // BLK

    def kernel(sel, x_hbm, *refs):
        outs, sems = refs[:pieces], refs[pieces]
        copies = []
        for i in range(picked):
            at = pl.ds(pl.multiple_of(lax.rem(sel[i], block_count) * BLK, BLK), BLK)
            for p in range(pieces):
                copies.append(
                    pltpu.make_async_copy(
                        x_hbm.at[at, p * w : (p + 1) * w],
                        outs[p].at[i * BLK : (i + 1) * BLK, :],
                        sems.at[i, p],
                    )
                )
        for c in copies:
            c.start()
        for c in copies:
            c.wait()

    return pl.pallas_call(
        kernel,
        out_shape=[sds((picked * BLK, w), BF)] * pieces,
        in_specs=[SMEM, HBM],
        out_specs=[VMEM] * pieces,
        scratch_shapes=[pltpu.SemaphoreType.DMA((picked, pieces))],
        cost_estimate=cost(1 << 20, 4 * picked * BLK * width),
        compiler_params=params(8),
        name="pick",
    )(in_hbm(sel_blocks), in_hbm(resid))


def stage_weights(after, arrays):
    count = len(arrays)

    def kernel(*refs):
        ins, outs, sems = refs[1 : 1 + count], refs[1 + count : 1 + 2 * count], refs[1 + 2 * count]
        copies = [
            pltpu.make_async_copy(a, b, sems.at[i]) for i, (a, b) in enumerate(zip(ins, outs))
        ]
        for c in copies:
            c.start()
        for c in copies:
            c.wait()

    return pl.pallas_call(
        kernel,
        out_shape=[sds(a.shape, a.dtype) for a in arrays],
        in_specs=[pl.BlockSpec(memory_space=pl.ANY)] + [HBM] * count,
        out_specs=[VMEM] * count,
        scratch_shapes=[pltpu.SemaphoreType.DMA((count,))],
        cost_estimate=cost(1 << 30, sum(a.size * a.dtype.itemsize for a in arrays)),
        compiler_params=params(4),
        name="stage_weights",
    )(after, *map(in_hbm, arrays))


def rotate_half(x, cos2, sin2):
    return x * cos2 + pltpu.roll(x, HEAD_WIDTH // 2, 1) * sin2


def ring_of(n):
    return list(range(0, 1)) + list(range(1, n, 2)) + list(range(2, n, 2))[::-1]


def look_up(table, index):
    out = jnp.int32(table[0])
    for i, value in enumerate(table[1:], 1):
        out = jnp.where(index == i, jnp.int32(value), out)
    return out


def at_offset(offset, n):
    ring = ring_of(n)
    place = look_up([ring.index(i) for i in range(n)], lax.axis_index("tp"))
    return look_up(ring, lax.rem(place + offset % n, n))


def piece_index(stage, k, n, chains):
    return at_offset(-stage if k % 2 == 0 else stage, n) * chains + k


def accumulate(stage, n, pieces, gain, router, weights, state, share):
    count = len(pieces)
    rows, w = pieces[0].shape
    wq, wk, _ = weights
    nq, nk = wq.shape[1], wk.shape[1]
    features = gain.shape[1]
    held = 0 if state is None else len(state)

    def kernel(*refs):
        xs = refs[:count]
        gain_ref, router_ref, wqr, wkr, wvr = refs[count : count + 5]
        before = refs[count + 5 : count + 5 + held]
        q_out, k_out, v_out, ss_out, gd_out, own_out = refs[count + 5 + held :]
        offsets = [
            pl.multiple_of(piece_index(stage, p, n, count) * w, w) for p in range(count)
        ]
        first = pl.multiple_of(lax.axis_index("tp") * share, share)
        xg = []
        ss = gd = None
        for p in range(count):
            at = pl.ds(offsets[p], w)
            x = xs[p][...].astype(F32)
            a = jnp.sum(x * x, axis=1, keepdims=True)
            b = jnp.sum(x * router_ref[:, at], axis=1, keepdims=True)
            ss = a if ss is None else ss + a
            gd = b if gd is None else gd + b
            xg.append((x * gain_ref[:, at]).astype(BF))
            own_out[:, at] = xs[p][pl.ds(first, share), :]
        for ref, out, weight in ((0, q_out, wqr), (1, k_out, wkr), (2, v_out, wvr)):
            total = before[ref][...] if held else None
            for p in range(count):
                d = jnp.dot(xg[p], weight[pl.ds(offsets[p], w), :], preferred_element_type=F32)
                total = d if total is None else total + d
            out[...] = total
        ss_out[...] = ss + before[3][...] if held else ss
        gd_out[...] = gd + before[4][...] if held else gd

    shapes = [
        sds((rows, nq), F32),
        sds((rows, nk), F32),
        sds((rows, nk), F32),
        sds((rows, 1), F32),
        sds((rows, 1), F32),
        sds((share, features), BF),
    ]
    return pl.pallas_call(
        kernel,
        out_shape=shapes,
        in_specs=[VMEM] * (count + 5 + held),
        out_specs=[VMEM] * 6,
        input_output_aliases={count + 5 + i: i for i in range(held)},
        cost_estimate=cost(2 * rows * w * count * (nq + 2 * nk), 2 * count * w * (nq + 2 * nk)),
        compiler_params=params(16),
        name="accumulate",
    )(*pieces, gain, router, *weights, *(state or ()))


def finish_kv(stage, n, pieces, gain, router, weights, state, cos2, sin2):
    count = len(pieces)
    rows, w = pieces[0].shape
    _, wk, wv = weights
    nk = wk.shape[1]
    features = gain.shape[1]

    def kernel(*refs):
        xs = refs[:count]
        gain_ref, router_ref, wkr, wvr, ka, va, ssa, gda, cos_ref, sin_ref = refs[
            count : count + 10
        ]
        kv_out, inv_out, gate_out = refs[count + 10 :]
        offsets = [
            pl.multiple_of(piece_index(stage, p, n, count) * w, w) for p in range(count)
        ]
        ss, gd = ssa[...], gda[...]
        xg = []
        for p in range(count):
            at = pl.ds(offsets[p], w)
            x = xs[p][...].astype(F32)
            ss += jnp.sum(x * x, axis=1, keepdims=True)
            gd += jnp.sum(x * router_ref[:, at], axis=1, keepdims=True)
            xg.append((x * gain_ref[:, at]).astype(BF))
        inv = jnp.broadcast_to(lax.rsqrt(ss * (1.0 / features) + norm_eps), (rows, HEAD_WIDTH))
        inv_out[...] = inv
        gate_out[...] = jnp.broadcast_to(1.0 / (1.0 + jnp.exp(-gd)), gate_out.shape)
        k, v = ka[...], va[...]
        for p in range(count):
            at = pl.ds(offsets[p], w)
            k += jnp.dot(xg[p], wkr[at, :], preferred_element_type=F32)
            v += jnp.dot(xg[p], wvr[at, :], preferred_element_type=F32)
        cos, sin = cos_ref[...] * inv, sin_ref[...] * inv
        for h in range(nk // HEAD_WIDTH):
            at = slice(h * HEAD_WIDTH, (h + 1) * HEAD_WIDTH)
            to = slice(nk + h * HEAD_WIDTH, nk + (h + 1) * HEAD_WIDTH)
            kv_out[:, at] = rotate_half(k[:, at], cos, sin).astype(BF)
            kv_out[:, to] = (v[:, at] * inv).astype(BF)

    return pl.pallas_call(
        kernel,
        out_shape=[
            sds((rows, 2 * nk), BF),
            sds((rows, HEAD_WIDTH), F32),
            sds((rows, HEAD_WIDTH), F32),
        ],
        in_specs=[VMEM] * (count + 10),
        out_specs=[VMEM] * 3,
        cost_estimate=cost(4 * rows * w * count * nk, 4 * count * w * nk),
        compiler_params=params(8),
        name="finish_kv",
    )(*pieces, gain, router, wk, wv, state[1], state[2], state[3], state[4], cos2, sin2)


def finish_q(stage, n, pieces, gain, weights, state, inv, cos2, sin2, share):
    count = len(pieces)
    rows, w = pieces[0].shape
    wq = weights[0]
    nq = wq.shape[1]
    features = gain.shape[1]

    def kernel(*refs):
        xs = refs[:count]
        gain_ref, wqr, qa, _, inv_ref, cos_ref, sin_ref = refs[count : count + 7]
        q_out, own_out = refs[count + 7 :]
        offsets = [
            pl.multiple_of(piece_index(stage, p, n, count) * w, w) for p in range(count)
        ]
        first = pl.multiple_of(lax.axis_index("tp") * share, share)
        xg = []
        for p in range(count):
            at = pl.ds(offsets[p], w)
            xg.append((xs[p][...].astype(F32) * gain_ref[:, at]).astype(BF))
            own_out[:, at] = xs[p][pl.ds(first, share), :]
        factor = inv_ref[...] * score_scale
        cos, sin = cos_ref[...] * factor, sin_ref[...] * factor
        for h in range(0, nq, 2 * HEAD_WIDTH):
            both = slice(h, h + 2 * HEAD_WIDTH)
            q = qa[:, both]
            for p in range(count):
                q += jnp.dot(
                    xg[p], wqr[pl.ds(offsets[p], w), both], preferred_element_type=F32
                )
            for i in range(2):
                at = slice(i * HEAD_WIDTH, (i + 1) * HEAD_WIDTH)
                to = slice(h + i * HEAD_WIDTH, h + (i + 1) * HEAD_WIDTH)
                q_out[:, to] = rotate_half(q[:, at], cos, sin).astype(BF)

    return pl.pallas_call(
        kernel,
        out_shape=[sds((rows, nq), BF), sds((share, features), BF)],
        in_specs=[VMEM] * (count + 7),
        out_specs=[VMEM] * 2,
        input_output_aliases={count + 3: 1},
        cost_estimate=cost(2 * rows * w * count * nq, 2 * count * w * nq),
        compiler_params=params(12),
        name="finish_q",
    )(*pieces, gain, wq, state[0], state[5], inv, cos2, sin2)


def attend(q, blocks, w_out, share, segments, dtypes, width=None, keep=False):
    n = lax.axis_size("tp")
    rows, nq = q.shape
    heads = nq // HEAD_WIDTH
    nk = blocks[0].shape[1] // 2
    kv_heads = nk // HEAD_WIDTH
    group = heads // kv_heads
    sizes = [seg[2] for seg in segments]
    bases = [sum(sizes[:i]) for i in range(len(sizes))]
    part = sum(sizes)
    spans = len(blocks)
    taken = group
    while taken % 2 == 0 and spans * rows * taken * part * 4 > 16 << 20:
        taken //= 2
    tall = taken * part
    model = width or w_out.shape[1]
    cw = 1024 if model % 1024 == 0 else model
    count = len(segments)
    groups = []
    bit = 1
    while bit < spans:
        for k in range(bit, 2 * bit, 4):
            groups.append((bit, range(k, min(k + 4, 2 * bit))))
        bit *= 2

    def kernel(*refs):
        q_ref = refs[0]
        kvs = refs[1 : 1 + spans]
        w_ref = refs[1 + spans]
        outs = refs[2 + spans : 2 + spans + count]
        qs, vs, sc, m_ref, acc, att = refs[-6:]
        me = lax.axis_index("ctx")
        starts = [
            pl.multiple_of(at_offset(off, n) * share + lo, math.gcd(share, lo) if lo else share)
            for off, lo, size in segments
        ]
        for k in range(spans):
            vs[k, :, HEAD_WIDTH:] = jnp.ones((rows, HEAD_WIDTH), BF)
        for base in range(0, heads, taken):
            kh = base // group
            for h in range(taken):
                col = (base + h) * HEAD_WIDTH
                for d in range(count):
                    to = h * part + bases[d]
                    qs[to : to + sizes[d], :] = q_ref[
                        pl.ds(starts[d], sizes[d]), col : col + HEAD_WIDTH
                    ]
            k_at = slice(kh * HEAD_WIDTH, (kh + 1) * HEAD_WIDTH)
            v_at = slice(nk + kh * HEAD_WIDTH, nk + (kh + 1) * HEAD_WIDTH)

            def score(k):
                return lax.dot_general(
                    qs[...],
                    kvs[k][:, k_at],
                    (((1,), (1,)), ((), ())),
                    preferred_element_type=F32,
                )

            def top(m, s):
                for i in range(rows // HEAD_WIDTH):
                    m = jnp.maximum(m, s[:, i * HEAD_WIDTH : (i + 1) * HEAD_WIDTH])
                return m

            def scores_of(span_group):
                m = m_ref[...]
                for k in span_group:
                    s = score(k)
                    sc[k] = s
                    m = top(m, s)
                m_ref[...] = m

            def weigh(span_group):
                m = m_ref[...]
                total = None
                for k in span_group:
                    vs[k, :, :HEAD_WIDTH] = kvs[k][:, v_at]
                    p = jnp.concatenate(
                        [
                            jnp.exp2(sc[k, :, i * HEAD_WIDTH : (i + 1) * HEAD_WIDTH] - m).astype(BF)
                            for i in range(rows // HEAD_WIDTH)
                        ],
                        axis=1,
                    )
                    d = jnp.dot(p, vs[k], preferred_element_type=F32)
                    total = d if total is None else total + d
                return total

            own_rows = jnp.concatenate(
                [lax.broadcasted_iota(jnp.int32, (size, 1), 0) + s for s, size in zip(starts, sizes)]
                * taken,
                axis=0,
            )
            key = lax.broadcasted_iota(jnp.int32, (tall, rows), 1)
            s = jnp.where(key <= own_rows, score(0), -1e30)
            sc[0] = s
            m_ref[...] = top(s[:, :HEAD_WIDTH], s)
            for bit, span_group in groups:

                @pl.when((me & bit) != 0)
                def _():
                    scores_of(span_group)

            m_ref[...] = jnp.broadcast_to(
                jnp.max(m_ref[...], axis=1, keepdims=True), m_ref.shape
            )
            acc[...] = weigh([0])
            for bit, span_group in groups:

                @pl.when((me & bit) != 0)
                def _():
                    acc[...] += weigh(span_group)

            done = (acc[:, :HEAD_WIDTH] / acc[:, HEAD_WIDTH:]).astype(BF)
            for h in range(taken):
                col = (base + h) * HEAD_WIDTH
                att[:, col : col + HEAD_WIDTH] = done[h * part : (h + 1) * part, :]
        if keep:
            refs[2 + spans + count][...] = att[...]
        for i in range(model // cw):
            at = slice(i * cw, (i + 1) * cw)
            proj = jnp.dot(att[...], w_ref[:, at], preferred_element_type=F32)
            for d in range(count):
                piece = proj[bases[d] : bases[d] + sizes[d], :]
                outs[d][:, at] = piece.astype(outs[d].dtype)

    return pl.pallas_call(
        kernel,
        out_shape=[sds((size, model), dt) for size, dt in zip(sizes, dtypes)]
        + [sds((part, nq), BF)] * keep,
        in_specs=[VMEM] * (2 + spans),
        out_specs=[VMEM] * (count + keep),
        scratch_shapes=[
            pltpu.VMEM((tall, HEAD_WIDTH), BF),
            pltpu.VMEM((spans, rows, 2 * HEAD_WIDTH), BF),
            pltpu.VMEM((spans, tall, rows), F32),
            pltpu.VMEM((tall, HEAD_WIDTH), F32),
            pltpu.VMEM((tall, 2 * HEAD_WIDTH), F32),
            pltpu.VMEM((part, nq), BF),
        ],
        cost_estimate=cost(
            4 * part * nq * rows * spans + 2 * part * nq * model,
            2 * nq * model + 2 * spans * rows * nk,
        ),
        compiler_params=params(10 + spans * tall * rows * 4 // (1 << 20)),
        name="attend",
    )(q, *blocks, w_out)


def project(att, w_out, first):
    rows, nq = att.shape
    width = w_out.shape[1] - first
    step = 1024 if width % 1024 == 0 else width

    def kernel(att_ref, w_ref, out):
        for at in range(0, width, step):
            out[:, at : at + step] = jnp.dot(
                att_ref[...],
                w_ref[:, first + at : first + at + step],
                preferred_element_type=F32,
            ).astype(BF)

    return pl.pallas_call(
        kernel,
        out_shape=sds((rows, width), BF),
        in_specs=[VMEM] * 2,
        out_specs=VMEM,
        cost_estimate=cost(2 * rows * nq * width, 2 * nq * width),
        compiler_params=params(8),
        name="project",
    )(att, w_out)


def combine(own, gate, got, places, mine):
    share, model = own.shape
    count = len(got)

    def kernel(own_ref, gate_ref, mine_ref, *refs):
        gs, out = refs[:count], refs[count]
        first = pl.multiple_of(lax.axis_index("tp") * share, share)
        g = gate_ref[pl.ds(first, share), 0:1]
        for i, (row, column) in enumerate(places):
            at = slice(row, row + got[i].shape[0])
            to = slice(column, column + got[i].shape[1])
            proj = gs[i][...].astype(F32) + mine_ref[at, to]
            out[at, to] = (own_ref[at, to].astype(F32) + g[at, :] * proj).astype(BF)

    return pl.pallas_call(
        kernel,
        out_shape=sds((share, model), BF),
        in_specs=[VMEM] * (3 + count),
        out_specs=VMEM,
        cost_estimate=cost(1 << 20, 8 * share * model),
        compiler_params=params(8),
        name="combine",
    )(own, gate, mine, *got)


def on_device(resid, sel_blocks, norm_gain, router_weight, w_query, w_key, value_projection, w_out):
    picked = sel_blocks.shape[0]
    n = lax.axis_size("tp")
    spans = lax.axis_size("ctx")
    rows = picked * BLK
    share = rows // n
    weights = (w_query, w_key, value_projection)
    ring = ring_of(n)
    up = [(ring[i], ring[(i + 1) % n]) for i in range(n)]
    down = [(ring[i], ring[i - 1]) for i in range(n)]
    ways = [up, down] * GATHER_WAYS

    positions = (sel_blocks[:, None] * BLK + jnp.arange(BLK, dtype=jnp.int32)[None, :]).reshape(rows)
    half = HEAD_WIDTH // 2
    freqs = jnp.exp(jnp.arange(half, dtype=F32) * (-2.0 * math.log(rope_base) / HEAD_WIDTH))
    angles = positions.astype(F32)[:, None] * freqs[None, :]
    cos, sin = jnp.cos(angles), jnp.sin(angles)
    cos2 = jnp.concatenate([cos, cos], axis=1)
    sin2 = jnp.concatenate([-sin, sin], axis=1)
    gain = norm_gain.reshape(1, -1)
    router = router_weight.reshape(1, -1)

    stages = [pick_rows(resid, sel_blocks, len(ways))]
    *weights, gain, router = stage_weights(stages[0][0], [*weights, gain, router])
    tie = gain
    state = None
    for s in range(n - 1):
        held = [lax.ppermute(b, "tp", way) for b, way in zip(stages[s], ways)]
        if s:
            state = accumulate(s - 1, n, stages[s - 1], gain, router, weights, state, share)
            tie = state[3]
        if s < n - 2:
            held = [lax.optimization_barrier((b, tie))[0] for b in held]
        stages.append(held)
    state = accumulate(n - 2, n, stages[n - 2], gain, router, weights, state, share)
    last = stages[n - 1]
    kv, inv, gate = finish_kv(n - 1, n, last, gain, router, weights, state, cos2, sin2)

    blocks = [None] * spans
    blocks[0] = kv
    for k in range(2, spans, 2):
        blocks[k] = lax.ppermute(kv, "ctx", [(i, i ^ k) for i in range(spans)])
    q, own = finish_q(n - 1, n, last, gain, weights, state, inv, cos2, sin2, share)
    for k in range(0, spans, 2):
        block = blocks[k]
        if k:
            block = lax.optimization_barrier((block, own))[0]
        blocks[k + 1] = lax.ppermute(block, "ctx", [(i, i ^ 1) for i in range(spans)])

    chains = 2 * SCATTER_WAYS
    size = share // chains
    out_ways = [down, up] * SCATTER_WAYS

    def segment(step, k):
        return (1 + step if k % 2 == 0 else n - 1 - step, k * size, size)

    early = w_out.shape[1] // 4
    first_part, att = attend(q, blocks, w_out, share, [segment(0, 0)], [BF], width=early, keep=True)
    second_part = project(att, w_out, early)
    q_next = lax.optimization_barrier((q, second_part))[0]
    (other,) = attend(q_next, blocks, w_out, share, [segment(0, 1)], [BF])
    q_next = lax.optimization_barrier((q, other))[0]
    near = [first_part, second_part, other]
    out_ways = [out_ways[0], out_ways[0], out_ways[1]]
    places = [(0, 0), (0, early), (size, 0)]
    later = [segment(s, k) for s in range(1, n - 1) for k in range(chains)]
    far = attend(q_next, blocks, w_out, share, later + [(0, 0, share)], [F32] * (len(later) + 1))
    moving = near
    for s in range(1, n):
        for k, way in enumerate(out_ways):
            moving[k] = lax.ppermute(moving[k], "tp", way)
        if s < n - 1:
            one, two = far[(s - 1) * chains : s * chains]
            mine = [one[:, :early], one[:, early:], two]
            for k, part in enumerate(mine):
                moving[k] = (moving[k].astype(F32) + part).astype(BF)
    return combine(own, gate, moving, places, far[-1])


def solution(mesh):
    return jax.shard_map(
        on_device,
        mesh=mesh,
        in_specs=(
            P("ctx", "tp"),
            P("ctx"),
            P(),
            P(),
            P(None, "tp"),
            P(None, "tp"),
            P(None, "tp"),
            P("tp", None),
        ),
        out_specs=P(("ctx", "tp"), None),
        check_vma=False,
    )
```
